256 devices in a mesh: seq: 8 (over x_lo, y), dp: 32 (over x_hi, z, core).
Axes of the slice: x: 4 (x_hi: 2, x_lo: 2; x = x_hi * 2 + x_lo), y: 4, z: 8, core: 2. Of those that a mesh axis runs over, the one named last changes fastest.
Arguments:
- tokens_in: bfloat16 [32, 2048, 2560], P('dp', 'seq'), may hold values from -6 to 6
- step_raw: bfloat16 [32, 2048, 40], P('dp', 'seq'), may hold values from -3 to 3
- input_map: bfloat16 [32, 2048, 128], P('dp', 'seq'), may hold values from -1.796875 to 1.796875
- output_map: bfloat16 [32, 2048, 128], P('dp', 'seq'), may hold values from -1.796875 to 1.796875
- decay_log: float32 [40], replicated
- skip_gain: float32 [40], replicated, may hold values from 0.5 to 1.5
- step_bias: float32 [40], replicated, may hold values from -4.7 to -2.2
- grad_out: bfloat16 [32, 2048, 2560], P('dp', 'seq'), may hold values from -6 to 6
Outputs:
- grad_tokens: bfloat16 [32, 2048, 2560], P('dp', 'seq')
- grad_steps: float32 [32, 2048, 40], P('dp', 'seq')
- grad_input_map: float32 [32, 2048, 128], P('dp', 'seq')
- grad_output_map: float32 [32, 2048, 128], P('dp', 'seq')
- grad_decay_log: float32 [40], replicated
- grad_skip_gain: float32 [40], replicated
- grad_step_bias: float32 [40], replicated
The draws below stay inside these ranges and needn't reach their ends.
All inputs are finite; a program needn't handle non-finite values.
Results may differ from the reference program's by a relative error of at most 0.001.
Values may be sent and summed in bfloat16 or wider, within the bound.
No kernel may reach another device: no remote copies, remote signals or barrier semaphores. Data moves between devices by JAX's collectives and lax.ppermute only.
A program may use at most 192 MiB of HBM per device.

```python
import math
import jax
import jax.numpy as jnp
from jax import lax

HEADS = 40
HEADDIM = 64
STATE = 128
SPAN = 256
HEAD_BLOCK = 8
TOK_DEV = 256
LENGTH = 2048
GROUPS = 32


def head_rates(key):
    slow_pick = jax.random.randint(jax.random.fold_in(key, 101), (HEADS,), 0, 10)
    slow_heads = slow_pick < 5
    slow_rate = jnp.exp(jax.random.uniform(jax.random.fold_in(key, 102), (HEADS,), jnp.float32, math.log(0.1), math.log(1.5))) / LENGTH
    fast_rate = jnp.exp(jax.random.uniform(jax.random.fold_in(key, 103), (HEADS,), jnp.float32, math.log(0.02), math.log(0.1)))
    base_step = jnp.exp(jax.random.uniform(jax.random.fold_in(key, 104), (HEADS,), jnp.float32, math.log(0.01), math.log(0.1)))
    return (jnp.where(slow_heads, slow_rate, fast_rate), base_step)


def draw_decay_log(key, part):
    per_token, base_step = head_rates(key)
    return jnp.log(per_token / base_step)


def draw_step_bias(key, part):
    per_token, base_step = head_rates(key)
    return jnp.log(jnp.expm1(base_step))


def draw_step_raw(key, part):
    noise_key = jax.random.fold_in(key, 201)
    noise = 0.5 * jax.random.truncated_normal(noise_key, -4.0, 4.0, (GROUPS, LENGTH, HEADS), jnp.float32)
    offsets = jax.random.uniform(jax.random.fold_in(key, 202), (GROUPS, LENGTH // TOK_DEV, HEADS), jnp.float32, -0.7, 0.7)
    return (noise + jnp.repeat(offsets, TOK_DEV, axis=1)).astype(jnp.bfloat16)


def block_levels(own_key, dims, pieces, smallest, top_value):
    def one(position, blocks):
        steps = jax.random.uniform(jax.random.fold_in(jax.random.fold_in(own_key, 6), position), (blocks,), jnp.float32, smallest / len(pieces), top_value / len(pieces))
        return jnp.repeat(jnp.exp(steps), dims[position] // blocks).reshape((-1,) + (1,) * (len(dims) - position - 1))

    gain = one(*pieces[0])
    for cut in pieces[1:]:
        gain = gain * one(*cut)
    return gain


def normal_values(key, dims, scale, most, pieces=(), kind=jnp.bfloat16):
    drawn = jax.random.normal(key, dims, jnp.float32) * scale
    if len(pieces) > 0:
        drawn = block_levels(key, dims, pieces, -0.22, 0.18) * drawn
    return jnp.clip(drawn, min=-most, max=most).astype(kind)


def setup_inputs(seed: int = 0) -> dict:
    keys = jax.random.split(jax.random.key(seed), 9)
    return {
        "tokens_in": normal_values(keys[0], (GROUPS, LENGTH, HEADS * HEADDIM), 1.0, 6.0, ((0, 32), (1, 8))),
        "step_raw": draw_step_raw(jax.random.fold_in(keys[8], 71), 0),
        "input_map": normal_values(keys[2], (GROUPS, LENGTH, STATE), 0.3, 1.796875, ((0, 32), (1, 8))),
        "output_map": normal_values(keys[3], (GROUPS, LENGTH, STATE), 0.3, 1.796875, ((0, 32), (1, 8))),
        "decay_log": draw_decay_log(jax.random.fold_in(keys[8], 71), 0),
        "skip_gain": jnp.clip(jax.random.uniform(keys[5], (HEADS,), jnp.float32, 0.5, 1.5), 0.5, 1.5),
        "step_bias": draw_step_bias(jax.random.fold_in(keys[8], 71), 0),
        "grad_out": normal_values(keys[7], (GROUPS, LENGTH, HEADS * HEADDIM), 1.0, 6.0, ((0, 32), (1, 8))),
    }


highest = lax.Precision.HIGHEST

def block_forward(head_block, input_rows, output_rows):
    values, step_sizes, decay_rates, skip_part, state_in = head_block
    length = values.shape[0]
    span_count = length // SPAN
    head_count = decay_rates.shape[0]
    head_width = values.shape[2]
    log_decay = -decay_rates[None, :] * step_sizes
    scaled = values * step_sizes[:, :, None]
    causal = lax.broadcasted_iota(jnp.int32, (SPAN, SPAN), 0) >= lax.broadcasted_iota(jnp.int32, (SPAN, SPAN), 1)

    def advance(state_now, span_item):
        span_in, span_decay, span_b, span_c = span_item
        running = jnp.cumsum(span_decay, axis=0)
        scores = jnp.dot(span_c, span_b.T, precision=highest)
        spread = running.T[:, :, None] - running.T[:, None, :]
        weights = jnp.exp(jnp.where(causal[None], spread, -jnp.inf)) * scores[None]
        inside = jnp.einsum('hts,shp->thp', weights, span_in, precision=highest)
        carried = jnp.einsum('tn,hpn->thp', span_c, state_now, precision=highest) * jnp.exp(running)[:, :, None]
        last_sum = running[-1]
        tail_weight = jnp.exp(last_sum[None, :] - running)
        fresh_state = jnp.einsum('shp,sn->hpn', span_in * tail_weight[:, :, None], span_b, precision=highest)
        return (jnp.exp(last_sum)[:, None, None] * state_now + fresh_state, inside + carried)
    span_items = (scaled.reshape(span_count, SPAN, head_count, head_width), log_decay.reshape(span_count, SPAN, head_count), input_rows.reshape(span_count, SPAN, -1), output_rows.reshape(span_count, SPAN, -1))
    state_out, outputs = lax.scan(advance, state_in, span_items)
    result = outputs.reshape(length, head_count, head_width) + skip_part[None, :, None] * values
    return (result, state_out)

def segment(values, raw_steps, input_rows, output_rows, decay_log, skip_gain, step_bias, state_in):
    length = values.shape[0]
    head_count = decay_log.shape[0]
    head_width = values.shape[1] // head_count
    state_size = input_rows.shape[1]
    per_block = math.gcd(HEAD_BLOCK, head_count)
    blocks = head_count // per_block
    step_sizes = jax.nn.softplus(raw_steps + step_bias[None, :])
    decay_rates = jnp.exp(decay_log)
    packed = (values.reshape(length, blocks, per_block, head_width).transpose(1, 0, 2, 3), step_sizes.reshape(length, blocks, per_block).transpose(1, 0, 2), decay_rates.reshape(blocks, per_block), skip_gain.reshape(blocks, per_block), state_in.reshape(blocks, per_block, head_width, state_size))
    results, finals = lax.map(lambda head_block: block_forward(head_block, input_rows, output_rows), packed)
    return (results.transpose(1, 0, 2, 3).reshape(length, head_count * head_width), finals.reshape(head_count, head_width, state_size))

def reference(tokens_in, step_raw, input_map, output_map, decay_log, skip_gain, step_bias, grad_out):
    zero_state = jnp.zeros((HEADS, HEADDIM, STATE), jnp.float32)

    def one_group(group_item):
        token_rows, raw_rows, input_rows, output_rows, cotangent = [member.astype(jnp.float32) for member in group_item]
        output, pullback = jax.vjp(lambda primals: segment(*primals, zero_state)[0], (token_rows, raw_rows, input_rows, output_rows, decay_log, skip_gain, step_bias))
        return pullback(cotangent)[0]
    gradients = lax.map(one_group, (tokens_in, step_raw, input_map, output_map, grad_out))
    factor = 1.0 / math.sqrt(GROUPS * LENGTH * HEADDIM)
    return (gradients[0].astype(jnp.bfloat16), gradients[1], gradients[2], gradients[3], lax.optimization_barrier(jnp.sum(gradients[4], axis=0)) * factor, lax.optimization_barrier(jnp.sum(gradients[5], axis=0)) * factor, lax.optimization_barrier(jnp.sum(gradients[6], axis=0)) * factor)
```

```python
import functools
import math

import jax
import jax.numpy as jnp
from jax import lax
from jax.experimental import pallas as pl
from jax.experimental.pallas import tpu as pltpu
from jax.sharding import Mesh
from jax.sharding import PartitionSpec as P

SEQ = ("seq_0", "seq_1")
DP = ("dp_0", "dp_1", "dp_2")
SEQ_DP = ("seq_0", "seq_1", "dp_0", "dp_1", "dp_2")

HI = lax.Precision.HIGHEST
F32 = jnp.float32
BF16 = jnp.bfloat16
LOG2E = math.log2(math.e)
T = 256
H = 40
HP = 2560
N = 128
DEV = 8
ROWS = N // DEV
STEP = 512
STEPS = HP // STEP
TOP = 14.0
TINY = 1e-30


def halves(value):
    high = value.astype(BF16)
    return high, (value - high.astype(F32)).astype(BF16)


def dot(a, b):
    return jnp.dot(a, b, preferred_element_type=F32)


def dot_nt(a, b):
    return lax.dot_general(a, b, (((1,), (1,)), ((), ())), preferred_element_type=F32)


def iota(shape, dim):
    return lax.broadcasted_iota(jnp.int32, shape, dim)


def by_pair(columns, k):
    first = iota((T, 128), 1) < 64
    return jnp.where(first, columns[:, k : k + 1], columns[:, k + 1 : k + 2])


def exponent(bound):
    return jnp.ceil(jnp.log2(bound + TINY)) - TOP


def prepare(raw_ref, dlog_ref, bias_ref, x_ref, g_ref, b_ref, c_ref,
            msg_ref, ext_ref, col_ref, row_ref, fin_ref, wide):
    v = raw_ref[...].astype(F32) + bias_ref[...]
    dt = jnp.maximum(v, 0.0) + jnp.log1p(jnp.exp(-jnp.abs(v)))
    la = -jnp.exp(dlog_ref[...]) * dt
    fin_ref[0] = dt
    fin_ref[1] = 1.0 / (1.0 + jnp.exp(-v))
    fin_ref[2] = la
    tri = (iota((T, T), 0) >= iota((T, T), 1)).astype(F32)
    run = jnp.dot(tri, la, precision=HI, preferred_element_type=F32) * LOG2E
    wide[...] = jnp.zeros_like(wide)
    wide[:, :H] = run
    row_ref[...] = wide[...].T[:H]
    total = run[T - 1 : T]
    into = jnp.exp2(total - run) * dt
    outof = jnp.exp2(run)
    shifted = run - jnp.log2(dt)
    for i in range(STEPS):
        at = slice(8 * i, 8 * i + 8)
        col_ref[i, :, 0:8] = shifted[:, at]
        col_ref[i, :, 8:16] = into[:, at]
        col_ref[i, :, 16:24] = outof[:, at]
    most_x = jnp.max(jnp.abs(x_ref[...]).astype(F32), keepdims=True)
    most_g = jnp.max(jnp.abs(g_ref[...]).astype(F32), keepdims=True)
    most_b = jnp.max(jnp.abs(b_ref[...]).astype(F32), keepdims=True)
    most_c = jnp.max(jnp.abs(c_ref[...]).astype(F32), keepdims=True)
    exp_s = exponent(most_x * most_b * jnp.sum(into, axis=0, keepdims=True))
    exp_g = exponent(most_g * most_c * jnp.sum(outof, axis=0, keepdims=True))
    keep = jnp.exp2(total)
    keep_a = keep.astype(BF16).astype(F32)
    keep_b = (keep - keep_a).astype(BF16).astype(F32)
    keep_c = keep - keep_a - keep_b
    ext_ref[...] = jnp.zeros_like(ext_ref)
    ext_ref[0:1, :H] = keep_a
    ext_ref[1:2, :H] = keep_b * 512.0
    ext_ref[2:3, :H] = keep_c * 262144.0
    ext_ref[3:4, :H] = exp_s
    ext_ref[4:5, :H] = exp_g
    into = into * jnp.exp2(-exp_s)
    outof = outof * jnp.exp2(-exp_g)
    for source, weight, maps, first in ((x_ref, into, b_ref, 0), (g_ref, outof, c_ref, ROWS)):
        left = maps[...].astype(F32).T.astype(BF16)
        for j in range(HP // 128):
            lanes = slice(128 * j, 128 * j + 128)
            high, low = halves(source[:, lanes].astype(F32) * by_pair(weight, 2 * j))
            state = dot(left, high) + dot(left, low)
            for o in range(DEV):
                msg_ref[o, first : first + ROWS, lanes] = state[ROWS * o : ROWS * o + ROWS]


def scan(got_ref, out_ref, ext_ref, wide):
    extra = [got_ref[j, 0:8, HP : HP + 128] for j in range(DEV)]
    keep = [e[0:1] + e[1:2] * (1.0 / 512.0) + e[2:3] * (1.0 / 262144.0) for e in extra]
    in_s = [jnp.exp2(e[3:4]) for e in extra]
    in_g = [jnp.exp2(e[4:5]) for e in extra]
    top = 2.0**TOP
    zero = jnp.zeros((1, 128), F32)
    bound_s, bound_g = [zero], [zero]
    for k in range(DEV - 1):
        bound_s.append(keep[k] * bound_s[-1] + in_s[k] * top)
        back = DEV - 1 - k
        bound_g.append(keep[back] * bound_g[-1] + in_g[back] * top)
    bound_g = bound_g[::-1]
    exp_s = [exponent(b) for b in bound_s]
    exp_g = [exponent(b) for b in bound_g]
    for k in range(DEV):
        ext_ref[k, 0:1] = exp_s[k]
        ext_ref[k, 1:2] = exp_g[k]
        ext_ref[k, 2:8] = jnp.zeros((6, 128), F32)
    rows = keep + in_s + in_g + [jnp.exp2(-e) for e in exp_s] + [jnp.exp2(-e) for e in exp_g]
    rows = jnp.concatenate(rows, axis=0)
    high, rest = rows.astype(BF16), rows
    rest = rest - high.astype(F32)
    mid = rest.astype(BF16)
    low = (rest - mid.astype(F32)).astype(BF16)
    parts = jnp.concatenate([high, mid, low], axis=0)
    count = 5 * DEV
    for c in range(STEPS):
        lanes = slice(STEP * c, STEP * c + STEP)
        hot = (iota((128, STEP), 0) == (iota((128, STEP), 1) + STEP * c) // 64).astype(BF16)
        spread = dot(parts, hot)
        wide[:, lanes] = spread[:count] + spread[count : 2 * count] + spread[2 * count :]
    for c in range(STEPS):
        lanes = slice(STEP * c, STEP * c + STEP)
        for first, scale, out, order in (
            (0, DEV, 3 * DEV, range(DEV)),
            (ROWS, 2 * DEV, 4 * DEV, range(DEV - 1, -1, -1)),
        ):
            held = jnp.zeros((ROWS, STEP), F32)
            for k in order:
                here = slice(first, first + ROWS)
                out_ref[k, here, lanes] = held * wide[out + k : out + k + 1, lanes]
                held = (
                    wide[k : k + 1, lanes] * held
                    + wide[scale + k : scale + k + 1, lanes] * got_ref[k, here, lanes]
                )


def inside(x_ref, g_ref, b_ref, c_ref, col_ref, row_ref,
           dx_ref, qrow_ref, qcol_ref, gx_ref, db_ref, dc_ref, score, total):
    i = pl.program_id(0)
    half = T // 2

    @pl.when(i == 0)
    def _():
        score[...] = dot_nt(b_ref[...], c_ref[...])
        total[...] = jnp.zeros_like(total)
        qcol_ref[...] = jnp.zeros_like(qcol_ref)

    causal = iota((half, T), 1) >= iota((half, T), 0)
    causal_end = iota((half, half), 1) >= iota((half, half), 0)
    lane = iota((half, 128), 1)
    for p in range(STEP // 128):
        lanes = slice(128 * p, 128 * p + 128)
        x = x_ref[:, lanes]
        g = g_ref[:, lanes]
        gx = jnp.sum(x.astype(F32) * g.astype(F32), axis=0, keepdims=True)
        gx_ref[:, lanes] = gx
        grads = []
        for q in range(2):
            k = 2 * p + q
            mine = iota((T, 128), 1) < 64 if q == 0 else iota((T, 128), 1) >= 64
            own = jnp.where(mine, x, jnp.zeros_like(x))
            at = 8 * i + k
            parts = []
            sums = []
            for start, width, keep in ((0, T, causal), (half, half, causal_end)):
                here = slice(start, start + half)
                later = slice(T - width, T)
                gap = row_ref[k : k + 1, later] - col_ref[0, here, k : k + 1]
                decay = jnp.exp2(jnp.where(keep, gap, -1e5))
                cross = dot_nt(own[here], g[later])
                weight = decay * score[here, later]
                high, low = halves(weight)
                parts.append(dot(high, g[later]) + dot(low, g[later]))
                total[here, later] += decay * cross
                pair = weight * cross
                sums.append(jnp.sum(pair, axis=0, keepdims=True))
                qcol_ref[here] += jnp.where(lane == at, jnp.sum(pair, axis=1, keepdims=True), 0.0)
            qrow_ref[k : k + 1, :half] = sums[0][:, :half]
            qrow_ref[k : k + 1, half:] = sums[0][:, half:] + sums[1]
            grads.append(parts)
        for s in range(2):
            dx_ref[half * s : half * s + half, lanes] = jnp.where(
                lane < 64, grads[0][s], grads[1][s]
            )

    @pl.when(i == STEPS - 1)
    def _():
        high, low = halves(total[...])
        db_ref[...] = dot(high, c_ref[...]) + dot(low, c_ref[...])
        high, low = halves(total[...].T)
        dc_ref[...] = dot(high, b_ref[...]) + dot(low, b_ref[...])


def outside(x_ref, g_ref, b_ref, c_ref, col_ref, got_ref, exp_ref, all_ref, dx_in_ref,
            db_in_ref, dc_in_ref, qrow_ref, qcol_ref, gx_ref, fin_ref, keep_ref, skip_ref,
            dx_ref, steps_ref, db_ref, dc_ref, par_ref, far_row, far_col, lane_sums, wide):
    i = pl.program_id(0)

    @pl.when(i == 0)
    def _():
        far_row[...] = jnp.zeros_like(far_row)
        far_col[...] = jnp.zeros_like(far_col)
        lane_sums[...] = jnp.zeros_like(lane_sums)
        db_ref[...] = db_in_ref[...]
        dc_ref[...] = dc_in_ref[...]

    state = jnp.concatenate([got_ref[o, 0:ROWS] for o in range(DEV)], axis=0)
    slope = jnp.concatenate([got_ref[o, ROWS : 2 * ROWS] for o in range(DEV)], axis=0)
    state_hi, state_lo = halves(state)
    slope_hi, slope_lo = halves(slope)
    seen = dot(c_ref[...], state_hi) + dot(c_ref[...], state_lo)
    back = dot(b_ref[...], slope_hi) + dot(b_ref[...], slope_lo)
    into = col_ref[0, :, 8:16] * jnp.exp2(exp_ref[0, 1:2])
    outof = col_ref[0, :, 16:24] * jnp.exp2(exp_ref[0, 0:1])
    hot = (iota((STEP, 128), 1) == iota((STEP, 128), 0) // 64 + 8 * i).astype(BF16)
    first = iota((1, 128), 1) < 64
    for p in range(STEP // 128):
        lanes = slice(128 * p, 128 * p + 128)
        x = x_ref[:, lanes].astype(F32)
        g = g_ref[:, lanes].astype(F32)
        ax = by_pair(into, 2 * p)
        eg = by_pair(outof, 2 * p) * g
        far = ax * back[:, lanes]
        at = 8 * i + 2 * p
        skip = jnp.where(first, skip_ref[at], skip_ref[at + 1])
        dx_ref[:, lanes] = (dx_in_ref[:, lanes] + far + skip * g).astype(BF16)
        ax = ax * x
        ax_hi, ax_lo = halves(ax)
        eg_hi, eg_lo = halves(eg)
        s_hi, s_lo = state_hi[:, lanes], state_lo[:, lanes]
        h_hi, h_lo = slope_hi[:, lanes], slope_lo[:, lanes]
        db_ref[...] += dot_nt(ax_hi, h_hi) + dot_nt(ax_hi, h_lo) + dot_nt(ax_lo, h_hi)
        dc_ref[...] += dot_nt(eg_hi, s_hi) + dot_nt(eg_hi, s_lo) + dot_nt(eg_lo, s_hi)
        high, low = halves(eg * seen[:, lanes])
        far_row[...] += dot(high, hot[lanes]) + dot(low, hot[lanes])
        high, low = halves(far * x)
        far_col[...] += dot(high, hot[lanes]) + dot(low, hot[lanes])
    both = jnp.concatenate(
        [jnp.sum(state * slope, axis=0, keepdims=True), gx_ref[...], jnp.zeros((6, STEP), F32)],
        axis=0,
    )
    lane_sums[...] += jnp.dot(both, hot.astype(F32), precision=HI, preferred_element_type=F32)

    @pl.when(i == STEPS - 1)
    def _():
        dt, gate, la = fin_ref[0], fin_ref[1], fin_ref[2]
        wide[...] = jnp.zeros_like(wide)
        wide[:H] = qrow_ref[...]
        near = wide[...].T - qcol_ref[...]
        since = (iota((T, T), 0) <= iota((T, T), 1)).astype(F32)
        before = (iota((T, T), 0) > iota((T, T), 1)).astype(F32)
        summed = jnp.dot(since, near + far_row[...], precision=HI, preferred_element_type=F32)
        summed += jnp.dot(before, far_col[...], precision=HI, preferred_element_type=F32)
        keep = keep_ref[0:1] + keep_ref[1:2] * (1.0 / 512.0) + keep_ref[2:3] * (1.0 / 262144.0)
        ends = keep * jnp.exp2(all_ref[0:1]) * lane_sums[0:1] * jnp.exp2(all_ref[1:2])
        dla = (summed + ends)[:, :H]
        rate = la * dla
        grad = gate * (((qcol_ref[...] + far_col[...])[:, :H] + rate) / dt)
        steps_ref[...] = grad
        par_ref[...] = jnp.zeros_like(par_ref)
        par_ref[0:1, :H] = jnp.sum(rate, axis=0, keepdims=True)
        par_ref[1:2, :H] = lane_sums[1:2, :H]
        par_ref[2:3, :H] = jnp.sum(grad, axis=0, keepdims=True)


def spec(shape, index=None):
    index = index or (lambda i: (0,) * len(shape))
    return pl.BlockSpec(shape, index)


def shape(*dims, dtype=F32):
    return jax.ShapeDtypeStruct(dims, dtype)


def packed(body, extra):
    extra = jnp.pad(extra, ((0, 0), (0, 2 * ROWS - 8), (0, 0)))
    return jnp.concatenate([body, extra], axis=2).astype(jnp.float16)


def exchange(message):
    return lax.all_to_all(message, SEQ, 0, 0, tiled=True)


def on_device(
    tokens_in, step_raw, input_map, output_map, decay_log, skip_gain, step_bias, grad_out
):
    x, raw, b, c, g = (m[0] for m in (tokens_in, step_raw, input_map, output_map, grad_out))
    ranks = lax.axis_size(SEQ) * lax.axis_size(DP)
    factor = 1.0 / math.sqrt(ranks * T * (HP // H))
    msg, ext, cols, rows, fin = pl.pallas_call(
        prepare,
        out_shape=(
            shape(DEV, 2 * ROWS, HP), shape(8, 128), shape(STEPS, T, 24), shape(H, T),
            shape(3, T, H),
        ),
        scratch_shapes=[pltpu.VMEM((T, 128), F32)],
        name="prepare",
    )(raw, decay_log[None], step_bias[None], x, g, b, c)
    got = exchange(packed(msg, jnp.broadcast_to(ext[None], (DEV, 8, 128))))

    lanes = spec((T, STEP), lambda i: (0, i))
    full = spec((T, N))
    cols_spec = spec((1, T, 24), lambda i: (i, 0, 0))
    gx_spec = spec((1, STEP), lambda i: (0, i))
    near_dx, qrow, qcol, gx, db, dc = pl.pallas_call(
        inside,
        grid=(STEPS,),
        in_specs=[lanes, lanes, full, full, cols_spec, spec((8, T), lambda i: (i, 0))],
        out_specs=[lanes, spec((8, T), lambda i: (i, 0)), full, gx_spec, full, full],
        out_shape=(
            shape(T, HP), shape(H, T), shape(T, 128), shape(1, HP), shape(T, N), shape(T, N),
        ),
        scratch_shapes=[pltpu.VMEM((T, T), F32), pltpu.VMEM((T, T), F32)],
        cost_estimate=pl.CostEstimate(
            flops=4_000_000_000, bytes_accessed=8_000_000, transcendentals=2_000_000
        ),
        name="inside",
    )(x, g, b, c, cols, rows)

    sent, sent_ext = pl.pallas_call(
        scan,
        out_shape=(shape(DEV, 2 * ROWS, HP), shape(DEV, 8, 128)),
        scratch_shapes=[pltpu.VMEM((5 * DEV, HP), F32)],
        name="scan",
    )(got.astype(F32))
    back = exchange(packed(sent, sent_ext)).astype(F32)
    scales = back[0, 0:8, HP:]
    by_step = scales[0:2, :H].reshape(2, STEPS, 8).transpose(1, 0, 2)

    dx, steps, db, dc, par = pl.pallas_call(
        outside,
        grid=(STEPS,),
        in_specs=[
            lanes, lanes, full, full, cols_spec,
            spec((DEV, 2 * ROWS, STEP), lambda i: (0, 0, i)),
            spec((1, 2, 8), lambda i: (i, 0, 0)), spec((8, 128)), lanes,
            full, full, spec((H, T)), spec((T, 128)), gx_spec, spec((3, T, H)), spec((8, 128)),
            pl.BlockSpec(memory_space=pltpu.SMEM),
        ],
        out_specs=[lanes, spec((T, H)), full, full, spec((8, 128))],
        out_shape=(
            shape(T, HP, dtype=BF16), shape(T, H), shape(T, N), shape(T, N), shape(8, 128),
        ),
        scratch_shapes=[
            pltpu.VMEM((T, 128), F32), pltpu.VMEM((T, 128), F32), pltpu.VMEM((8, 128), F32),
            pltpu.VMEM((128, T), F32),
        ],
        name="outside",
    )(x, g, b, c, cols, back, by_step, scales, near_dx, db, dc, qrow, qcol, gx, fin, ext,
      skip_gain)

    mine = par[0:3, :H].reshape(1, 3 * H)
    mine = jnp.pad(mine, ((0, 0), (0, 128 - 3 * H)))
    everyone = lax.all_to_all(
        jnp.broadcast_to(mine[None], (ranks, 1, 128)), SEQ_DP, 0, 0, tiled=True
    )
    total = jnp.sum(everyone, axis=(0, 1)) * factor
    return (
        dx[None], steps[None], db[None], dc[None],
        total[:H], total[H : 2 * H], total[2 * H : 3 * H],
    )


def build(split):
    held = P(DP, SEQ, None)
    return jax.shard_map(
        on_device,
        mesh=split,
        in_specs=(held, held, held, held, P(), P(), P(), held),
        out_specs=(held, held, held, held, P(), P(), P()),
        check_vma=False,
    )


def solution(mesh):
    return build(Mesh(mesh.devices.reshape(2, 4, 2, 8, 2), SEQ_DP))
```

```python
import functools
import math

import jax
import jax.numpy as jnp
from jax import lax
from jax.experimental import pallas as pl
from jax.experimental.pallas import tpu as pltpu
from jax.sharding import Mesh
from jax.sharding import PartitionSpec as P

SEQ = ("seq_0", "seq_1")
DP = ("dp_0", "dp_1", "dp_2")
SEQ_DP = ("seq_0", "seq_1", "dp_0", "dp_1", "dp_2")

HI = lax.Precision.HIGHEST
F32 = jnp.float32
BF16 = jnp.bfloat16
LOG2E = math.log2(math.e)
T = 256
H = 40
HP = 2560
N = 128
DEV = 8
ROWS = N // DEV
STEP = 512
STEPS = HP // STEP
TOP = 7.0
TINY = 1e-30


def halves(value):
    high = value.astype(BF16)
    return high, (value - high.astype(F32)).astype(BF16)


def dot(a, b):
    return jnp.dot(a, b, preferred_element_type=F32)


def dot_nt(a, b):
    return lax.dot_general(a, b, (((1,), (1,)), ((), ())), preferred_element_type=F32)


def exact(a, b):
    return jnp.dot(a, b, precision=HI, preferred_element_type=F32)


def iota(shape, dim):
    return lax.broadcasted_iota(jnp.int32, shape, dim)


def spread(columns, k, count):
    first = iota((T, 128), 1) < 64
    pairs = [
        jnp.where(first, columns[:, j : j + 1], columns[:, j + 1 : j + 2])
        for j in range(k, k + count, 2)
    ]
    return jnp.concatenate(pairs, axis=1)


def exponent(bound):
    return jnp.ceil(jnp.log2(bound + TINY)) - TOP


def prepare(raw_hbm, dlog_hbm, bias_hbm, x_hbm, g_hbm, b_hbm, c_hbm,
            msg_ref, scale_ref, ext_ref, col_ref, row_ref, fin_ref,
            raw_ref, dlog_ref, bias_ref, x_ref, g_ref, b_ref, c_ref, sems, wide, peaks):
    copies = [
        pltpu.make_async_copy(source, target, sems.at[k])
        for k, (source, target) in enumerate((
            (raw_hbm, raw_ref), (dlog_hbm, dlog_ref), (bias_hbm, bias_ref), (b_hbm, b_ref),
            (x_hbm, x_ref), (c_hbm, c_ref), (g_hbm, g_ref),
        ))
    ]
    for copy in copies:
        copy.start()
    for copy in copies[:3]:
        copy.wait()
    peaks[0:8] = jnp.zeros((8, 128), F32)
    peaks[0:1, :H] = jnp.exp(dlog_ref[...])
    peaks[1:2, :H] = bias_ref[...]
    heads = jnp.concatenate([peaks[0:8], jnp.zeros((120, 128), F32)], axis=0).T[:H]
    v = raw_ref[...].astype(F32) + heads[:, 1:2]
    dt = jnp.maximum(v, 0.0) + jnp.log1p(jnp.exp(-jnp.abs(v)))
    la = -heads[:, 0:1] * dt
    fin_ref[0] = dt
    fin_ref[1] = 1.0 / (1.0 + jnp.exp(-v))
    fin_ref[2] = la
    until = (iota((T, T), 0) <= iota((T, T), 1)).astype(F32)
    run = exact(la, until) * LOG2E
    row_ref[...] = run
    total = run[:, T - 1 : T]
    wide[0:H] = run - jnp.log2(dt)
    wide[H : 2 * H] = jnp.exp2(total - run) * dt
    wide[2 * H : 3 * H] = jnp.exp2(run)
    wide[3 * H :] = jnp.zeros((128 - 3 * H, T), F32)
    columns = wide[...].T
    for i in range(STEPS):
        for part in range(3):
            at = H * part + 8 * i
            col_ref[i, :, 8 * part : 8 * part + 8] = columns[:, at : at + 8]
    keep = columns[T - 1 : T, 2 * H : 3 * H]
    keep_a = keep.astype(BF16).astype(F32)
    keep_b = (keep - keep_a).astype(BF16).astype(F32)
    keep_c = keep - keep_a - keep_b
    ext_ref[...] = jnp.zeros_like(ext_ref)
    ext_ref[0:1, :H] = keep_a
    ext_ref[1:2, :H] = keep_b * 512.0
    ext_ref[2:3, :H] = keep_c * 262144.0
    peaks[...] = jnp.zeros_like(peaks)
    for r, (source, start, maps) in enumerate(((x_ref, H, b_ref), (g_ref, 2 * H, c_ref))):
        copies[3 + 2 * r].wait()
        copies[4 + 2 * r].wait()
        left = maps[...].astype(F32).T.astype(BF16)
        for j in range(HP // 256):
            lanes = slice(256 * j, 256 * j + 256)
            weight = spread(columns, start + 4 * j, 4)
            high, low = halves(source[:, lanes].astype(F32) * weight)
            state = dot(left, high) + dot(left, low)
            most = jnp.max(jnp.abs(state), axis=0, keepdims=True)
            peaks[24 * r + 2 * j : 24 * r + 2 * j + 1] = most[:, :128]
            peaks[24 * r + 2 * j + 1 : 24 * r + 2 * j + 2] = most[:, 128:]
            for o in range(DEV):
                msg_ref[o, ROWS * r : ROWS * r + ROWS, lanes] = state[ROWS * o : ROWS * o + ROWS]
    lane = iota((24, 128), 1)
    pair = 2 * iota((24, 128), 0)
    for r in range(2):
        most = peaks[24 * r : 24 * r + 24]
        even = exponent(jnp.max(jnp.where(lane < 64, most, 0.0), axis=1, keepdims=True))
        odd = exponent(jnp.max(jnp.where(lane < 64, 0.0, most), axis=1, keepdims=True))
        placed = jnp.where(lane == pair, even, jnp.where(lane == pair + 1, odd, 0.0))
        ext_ref[3 + r : 4 + r] = jnp.sum(placed, axis=0, keepdims=True)
        scale = jnp.exp2(-jnp.where(lane < 64, even, odd))
        for j in range(HP // 128):
            scale_ref[r : r + 1, 128 * j : 128 * j + 128] = scale[j : j + 1]


def scan(got_ref, extra_ref, out_ref, ext_ref, wide):
    extra = [extra_ref[j] for j in range(DEV)]
    keep = [e[0:1] + e[1:2] * (1.0 / 512.0) + e[2:3] * (1.0 / 262144.0) for e in extra]
    in_s = [jnp.exp2(e[3:4]) for e in extra]
    in_g = [jnp.exp2(e[4:5]) for e in extra]
    top = 2.0**TOP
    zero = jnp.zeros((1, 128), F32)
    bound_s, bound_g = [zero], [zero]
    for k in range(DEV - 1):
        bound_s.append(keep[k] * bound_s[-1] + in_s[k] * top)
        back = DEV - 1 - k
        bound_g.append(keep[back] * bound_g[-1] + in_g[back] * top)
    bound_g = bound_g[::-1]
    exp_s = [exponent(b) for b in bound_s]
    exp_g = [exponent(b) for b in bound_g]
    for k in range(DEV):
        ext_ref[k, 0:1] = exp_s[k]
        ext_ref[k, 1:2] = exp_g[k]
        ext_ref[k, 2:8] = jnp.zeros((6, 128), F32)
    rows = keep + in_s + in_g + [jnp.exp2(-e) for e in exp_s] + [jnp.exp2(-e) for e in exp_g]
    rows = jnp.concatenate(rows, axis=0)
    high = rows.astype(BF16)
    rest = rows - high.astype(F32)
    mid, low = halves(rest)
    parts = jnp.concatenate([high, mid, low], axis=0)
    count = 5 * DEV
    for c in range(STEPS):
        lanes = slice(STEP * c, STEP * c + STEP)
        hot = (iota((128, STEP), 0) == (iota((128, STEP), 1) + STEP * c) // 64).astype(BF16)
        over = dot(parts, hot)
        wide[:, lanes] = over[:count] + over[count : 2 * count] + over[2 * count :]
    for c in range(STEPS):
        lanes = slice(STEP * c, STEP * c + STEP)
        for first, scale, out, order in (
            (0, DEV, 3 * DEV, range(DEV)),
            (ROWS, 2 * DEV, 4 * DEV, range(DEV - 1, -1, -1)),
        ):
            held = jnp.zeros((ROWS, STEP), F32)
            for k in order:
                here = slice(first, first + ROWS)
                out_ref[k, here, lanes] = held * wide[out + k : out + k + 1, lanes]
                held = (
                    wide[k : k + 1, lanes] * held
                    + wide[scale + k : scale + k + 1, lanes] * got_ref[k, here, lanes]
                )


def inside(x_ref, g_ref, b_ref, c_ref, col_ref, row_ref,
           dx_ref, qrow_ref, qcol_ref, gx_ref, db_ref, dc_ref, score, total, qcol):
    i = pl.program_id(0)
    half = T // 2

    @pl.when(i == 0)
    def _():
        score[...] = dot_nt(b_ref[...], c_ref[...])
        total[...] = jnp.zeros_like(total)
        qcol[...] = jnp.zeros_like(qcol)

    causal = iota((half, T), 1) >= iota((half, T), 0)
    causal_end = iota((half, half), 1) >= iota((half, half), 0)
    lane = iota((half, 128), 1)
    for p in range(STEP // 128):
        lanes = slice(128 * p, 128 * p + 128)
        x = x_ref[:, lanes]
        g = g_ref[:, lanes]
        gx = jnp.sum(x.astype(F32) * g.astype(F32), axis=0, keepdims=True)
        gx_ref[:, lanes] = gx
        grads = []
        for q in range(2):
            k = 2 * p + q
            mine = iota((T, 128), 1) < 64 if q == 0 else iota((T, 128), 1) >= 64
            own = jnp.where(mine, x, jnp.zeros_like(x))
            at = 8 * i + k
            parts = []
            sums = []
            for start, width, keep in ((0, T, causal), (half, half, causal_end)):
                here = slice(start, start + half)
                later = slice(T - width, T)
                gap = row_ref[k : k + 1, later] - col_ref[0, here, k : k + 1]
                decay = jnp.exp2(jnp.where(keep, gap, -1e5))
                cross = dot_nt(own[here], g[later])
                weight = decay * score[here, later]
                high, low = halves(weight)
                parts.append(dot(high, g[later]) + dot(low, g[later]))
                total[here, later] += decay * cross
                pair = weight * cross
                sums.append(jnp.sum(pair, axis=0, keepdims=True))
                qcol[here] += jnp.where(lane == at, jnp.sum(pair, axis=1, keepdims=True), 0.0)
            qrow_ref[k : k + 1, :half] = sums[0][:, :half]
            qrow_ref[k : k + 1, half:] = sums[0][:, half:] + sums[1]
            grads.append(parts)
        for s in range(2):
            dx_ref[half * s : half * s + half, lanes] = jnp.where(
                lane < 64, grads[0][s], grads[1][s]
            )

    @pl.when(i == STEPS - 1)
    def _():
        high, low = halves(total[...])
        db_ref[...] = dot(high, c_ref[...]) + dot(low, c_ref[...])
        high, low = halves(total[...].T)
        dc_ref[...] = dot(high, b_ref[...]) + dot(low, b_ref[...])
        qcol_ref[...] = qcol[...].T[:H]


def entering(got_ref, first, i):
    lanes = slice(STEP * i, STEP * i + STEP)
    return jnp.concatenate([got_ref[o, first : first + ROWS, lanes] for o in range(DEV)], axis=0)


def outside(x_ref, g_ref, b_ref, c_ref, col_ref, got_ref, all_ref, qrow_ref, qcol_ref, gx_ref,
            fin_ref, keep_ref, dx_in_hbm, skip_ref,
            dx_hbm, steps_ref, par_ref,
            dx_in_ref, part_ref, dx_ref, sems, far_row, far_col):
    arrive = pltpu.make_async_copy(dx_in_hbm, dx_in_ref, sems.at[0])
    leave = pltpu.make_async_copy(dx_ref, dx_hbm, sems.at[1])
    arrive.start()
    first = iota((1, 128), 1) < 64
    lane_sums = jnp.zeros((8, 128), F32)
    for i in range(STEPS):
        whole = slice(STEP * i, STEP * i + STEP)
        state, slope = entering(got_ref, 0, i), entering(got_ref, ROWS, i)
        high, low = halves(state)
        seen = dot(c_ref[...], high) + dot(c_ref[...], low)
        high, low = halves(slope)
        back = dot(b_ref[...], high) + dot(b_ref[...], low)
        at = slice(8 * i, 8 * i + 8)
        into = col_ref[i, :, 8:16] * jnp.exp2(all_ref[1:2, at])
        outof = col_ref[i, :, 16:24] * jnp.exp2(all_ref[0:1, at])
        hot = (iota((STEP, 128), 1) == iota((STEP, 128), 0) // 64 + 8 * i).astype(BF16)
        row_parts, col_parts = [], []
        for p in range(STEP // 128):
            part = slice(128 * p, 128 * p + 128)
            lanes = slice(STEP * i + 128 * p, STEP * i + 128 * p + 128)
            x = x_ref[:, lanes].astype(F32)
            g = g_ref[:, lanes].astype(F32)
            far = spread(into, 2 * p, 2) * back[:, part]
            head = 8 * i + 2 * p
            skip = jnp.where(first, skip_ref[head], skip_ref[head + 1])
            part_ref[:, lanes] = far + skip * g
            row_parts.append(halves(spread(outof, 2 * p, 2) * g * seen[:, part]))
            col_parts.append(halves(far * x))
        for parts, sums in ((row_parts, far_row), (col_parts, far_col)):
            high = jnp.concatenate([p[0] for p in parts], axis=1)
            low = jnp.concatenate([p[1] for p in parts], axis=1)
            new = dot(high, hot) + dot(low, hot)
            sums[...] = new if i == 0 else sums[...] + new
        both = jnp.concatenate(
            [jnp.sum(state * slope, axis=0, keepdims=True), gx_ref[:, whole],
             jnp.zeros((6, STEP), F32)],
            axis=0,
        )
        lane_sums += exact(both, hot.astype(F32))
    arrive.wait()
    dx_ref[...] = (dx_in_ref[...] + part_ref[...]).astype(BF16)
    leave.start()
    dt, gate, la = fin_ref[0], fin_ref[1], fin_ref[2]
    rows, cols = far_row[...].T[:H], far_col[...].T[:H]
    since = (iota((T, T), 0) >= iota((T, T), 1)).astype(F32)
    before = (iota((T, T), 0) < iota((T, T), 1)).astype(F32)
    summed = exact(qrow_ref[...] - qcol_ref[...] + rows, since) + exact(cols, before)
    keep = keep_ref[0:1] + keep_ref[1:2] * (1.0 / 512.0) + keep_ref[2:3] * (1.0 / 262144.0)
    ends = keep * jnp.exp2(all_ref[0:1]) * lane_sums[0:1] * jnp.exp2(all_ref[1:2])
    ends = jnp.concatenate([ends, jnp.zeros((127, 128), F32)], axis=0).T[:H, 0:1]
    rate = la * (summed + ends)
    grad = gate * ((qcol_ref[...] + cols + rate) / dt)
    steps_ref[...] = grad
    ones = jnp.ones((8, T), F32)
    rate_sum, grad_sum = (
        lax.dot_general(
            ones, v, (((1,), (1,)), ((), ())), precision=HI, preferred_element_type=F32
        )[0:1]
        for v in (rate, grad)
    )
    mine = jnp.concatenate(
        [rate_sum, lane_sums[1:2, :H], grad_sum, jnp.zeros((1, 128 - 3 * H), F32)], axis=1
    )
    par_ref[...] = jnp.broadcast_to(mine[None], par_ref.shape)
    leave.wait()


def maps(x_hbm, g_hbm, col_hbm, db_hbm, dc_hbm, got_ref, all_ref, db_ref, dc_ref,
         x_ref, g_ref, col_ref, sems):
    copies = [
        pltpu.make_async_copy(source, target, sems.at[k])
        for k, (source, target) in enumerate((
            (col_hbm, col_ref), (x_hbm, x_ref), (g_hbm, g_ref), (db_hbm, db_ref), (dc_hbm, dc_ref),
        ))
    ]
    for copy in copies:
        copy.start()
    copies[0].wait()
    for k, (source, first, column, row, out) in enumerate((
        (x_ref, ROWS, 8, 1, db_ref), (g_ref, 0, 16, 0, dc_ref),
    )):
        copies[1 + k].wait()
        copies[3 + k].wait()
        for i in range(STEPS):
            weight = col_ref[i, :, column : column + 8]
            weight = weight * jnp.exp2(all_ref[row : row + 1, 8 * i : 8 * i + 8])
            rows = source[:, STEP * i : STEP * i + STEP].astype(F32)
            high, low = halves(spread(weight, 0, 8) * rows)
            other, rest = halves(entering(got_ref, first, i))
            out[...] += dot_nt(high, other) + dot_nt(high, rest) + dot_nt(low, other)


def spec(shape, index=None):
    index = index or (lambda i: (0,) * len(shape))
    return pl.BlockSpec(shape, index)


def shape(*dims, dtype=F32):
    return jax.ShapeDtypeStruct(dims, dtype)


def packed(body, extra):
    extra = jnp.pad(extra, ((0, 0), (0, 2 * ROWS - 8), (0, 0)))
    return jnp.concatenate([body * jnp.abs(body), extra], axis=2).astype(jnp.float16)


def unpacked(message):
    body = message[:, :, :HP].astype(F32)
    body = body * lax.rsqrt(jnp.maximum(jnp.abs(body), TINY))
    return near(body), message[:, 0:8, HP:].astype(F32)


def near(array):
    return pltpu.with_memory_space_constraint(array, pltpu.VMEM)


def far_off(*arrays):
    return [pltpu.with_memory_space_constraint(a, pltpu.HBM) for a in arrays]


def exchange(message):
    return lax.all_to_all(message, SEQ, 0, 0, tiled=True)


def on_device(
    tokens_in, step_raw, input_map, output_map, decay_log, skip_gain, step_bias, grad_out
):
    x, raw, b, c, g = (m[0] for m in (tokens_in, step_raw, input_map, output_map, grad_out))
    ranks = lax.axis_size(SEQ) * lax.axis_size(DP)
    factor = 1.0 / math.sqrt(ranks * T * (HP // H))
    vmem = pl.BlockSpec(memory_space=pltpu.VMEM)
    cost = pl.CostEstimate(
        flops=4_000_000_000, bytes_accessed=8_000_000, transcendentals=2_000_000
    )
    room = pltpu.CompilerParams(vmem_limit_bytes=24 * 1024 * 1024)
    msg, scale, ext, cols, rows, fin = pl.pallas_call(
        prepare,
        in_specs=(pl.BlockSpec(memory_space=pltpu.HBM),) * 7,
        out_shape=(
            pltpu.VMEM((DEV, 2 * ROWS, HP), F32), pltpu.VMEM((2, HP), F32),
            pltpu.VMEM((8, 128), F32), pltpu.HBM((STEPS, T, 24), F32), pltpu.HBM((H, T), F32),
            pltpu.HBM((3, H, T), F32),
        ),
        out_specs=(vmem,) * 6,
        scratch_shapes=[
            pltpu.VMEM((H, T), BF16), pltpu.VMEM((1, H), F32), pltpu.VMEM((1, H), F32),
            pltpu.VMEM((T, HP), BF16), pltpu.VMEM((T, HP), BF16), pltpu.VMEM((T, N), BF16),
            pltpu.VMEM((T, N), BF16), pltpu.SemaphoreType.DMA((7,)),
            pltpu.VMEM((128, T), F32), pltpu.VMEM((48, 128), F32),
        ],
        compiler_params=room,
        name="prepare",
    )(*far_off(raw.T, decay_log[None], step_bias[None], x, g, b, c))
    scale = jnp.broadcast_to(scale[:, None], (2, ROWS, HP)).reshape(2 * ROWS, HP)
    message = packed(msg * scale[None], jnp.broadcast_to(ext[None], (DEV, 8, 128)))
    got, got_ext = unpacked(exchange(message))

    lanes = spec((T, STEP), lambda i: (0, i))
    full = spec((T, N))
    heads = spec((H, T))
    cols_spec = spec((1, T, 24), lambda i: (i, 0, 0))
    gx_spec = spec((1, STEP), lambda i: (0, i))
    near_dx, qrow, qcol, gx, db, dc = pl.pallas_call(
        inside,
        grid=(STEPS,),
        in_specs=[lanes, lanes, full, full, cols_spec, spec((8, T), lambda i: (i, 0))],
        out_specs=[lanes, spec((8, T), lambda i: (i, 0)), heads, gx_spec, full, full],
        out_shape=(
            pltpu.HBM((T, HP), F32), pltpu.HBM((H, T), F32), pltpu.HBM((H, T), F32),
            pltpu.HBM((1, HP), F32), pltpu.HBM((T, N), F32), pltpu.HBM((T, N), F32),
        ),
        scratch_shapes=[
            pltpu.VMEM((T, T), F32), pltpu.VMEM((T, T), F32), pltpu.VMEM((T, 128), F32),
        ],
        cost_estimate=cost,
        compiler_params=room,
        name="inside",
    )(x, g, b, c, cols, rows)

    sent, sent_ext = pl.pallas_call(
        scan,
        in_specs=(vmem, vmem),
        out_shape=(pltpu.VMEM((DEV, 2 * ROWS, HP), F32), pltpu.VMEM((DEV, 8, 128), F32)),
        out_specs=(vmem, vmem),
        scratch_shapes=[pltpu.VMEM((5 * DEV, HP), F32)],
        compiler_params=room,
        name="scan",
    )(got, got_ext)
    back, scales = unpacked(exchange(packed(sent, sent_ext)))
    scales = scales[0]

    hbm = pl.BlockSpec(memory_space=pltpu.HBM)
    dx, steps, everyone = pl.pallas_call(
        outside,
        in_specs=[vmem] * 12 + [hbm, pl.BlockSpec(memory_space=pltpu.SMEM)],
        out_specs=[hbm, vmem, vmem],
        out_shape=(pltpu.HBM((T, HP), BF16), shape(H, T), shape(ranks, 1, 128)),
        scratch_shapes=[
            pltpu.VMEM((T, HP), F32), pltpu.VMEM((T, HP), F32), pltpu.VMEM((T, HP), BF16),
            pltpu.SemaphoreType.DMA((2,)),
            pltpu.VMEM((T, 128), F32), pltpu.VMEM((T, 128), F32),
        ],
        compiler_params=room,
        name="outside",
    )(near(x), near(g), near(b), near(c), near(cols), back, scales, near(qrow), near(qcol),
      near(gx), near(fin), near(ext), *far_off(near_dx), skip_gain)
    everyone = lax.all_to_all(everyone, SEQ_DP, 0, 0, tiled=True)
    db, dc = pl.pallas_call(
        maps,
        in_specs=[hbm] * 5 + [vmem] * 2,
        out_specs=[vmem] * 2,
        out_shape=(shape(T, N), shape(T, N)),
        scratch_shapes=[
            pltpu.VMEM((T, HP), BF16), pltpu.VMEM((T, HP), BF16),
            pltpu.VMEM((STEPS, T, 24), F32), pltpu.SemaphoreType.DMA((5,)),
        ],
        cost_estimate=cost,
        compiler_params=room,
        name="maps",
    )(*far_off(x, g, cols, db, dc), back, scales)
    total = jnp.sum(everyone, axis=(0, 1)) * factor
    return (
        dx[None], steps.T[None], db[None], dc[None],
        total[:H], total[H : 2 * H], total[2 * H : 3 * H],
    )


def build(split):
    held = P(DP, SEQ, None)
    return jax.shard_map(
        on_device,
        mesh=split,
        in_specs=(held, held, held, held, P(), P(), P(), held),
        out_specs=(held, held, held, held, P(), P(), P()),
        check_vma=False,
    )


def solution(mesh):
    return build(Mesh(mesh.devices.reshape(2, 4, 2, 8, 2), SEQ_DP))
```

```python
import functools
import math

import jax
import jax.numpy as jnp
from jax import lax
from jax.experimental import pallas as pl
from jax.experimental.pallas import tpu as pltpu
from jax.sharding import Mesh
from jax.sharding import PartitionSpec as P

SEQ = ("seq_0", "seq_1")
DP = ("dp_0", "dp_1", "dp_2")
SEQ_DP = ("seq_0", "seq_1", "dp_0", "dp_1", "dp_2")

F32 = jnp.float32
BF16 = jnp.bfloat16
LOG2E = math.log2(math.e)
T = 256
H = 40
HP = 2560
N = 128
DEV = 8
ROWS = N // DEV
STEP = 512
STEPS = HP // STEP
TOP = 7.0
TINY = 1e-30


def halves(value):
    high = value.astype(BF16)
    return high, (value - high.astype(F32)).astype(BF16)


def dot(a, b):
    return jnp.dot(a, b, preferred_element_type=F32)


def dot_nt(a, b):
    return lax.dot_general(a, b, (((1,), (1,)), ((), ())), preferred_element_type=F32)


def in_three(value):
    high = value.astype(BF16).astype(F32)
    mid = (value - high).astype(BF16).astype(F32)
    return jnp.concatenate([high, mid, value - high - mid], axis=0).astype(BF16)


def summed_by(value, zero_one):
    out = dot(in_three(value), zero_one)
    n = value.shape[0]
    return out[:n] + out[n : 2 * n] + out[2 * n :]


def iota(shape, dim):
    return lax.broadcasted_iota(jnp.int32, shape, dim)


def spread(columns, k, count):
    first = iota((T, 128), 1) < 64
    pairs = [
        jnp.where(first, columns[:, j : j + 1], columns[:, j + 1 : j + 2])
        for j in range(k, k + count, 2)
    ]
    return jnp.concatenate(pairs, axis=1)


def exponent(bound):
    return jnp.ceil(jnp.log2(bound + TINY)) - TOP


def prepare(raw_hbm, dlog_hbm, bias_hbm, x_hbm, g_hbm, b_hbm, c_hbm,
            msg_ref, scale_ref, ext_ref, col_ref, row_ref, fin_ref,
            raw_ref, dlog_ref, bias_ref, x_ref, g_ref, b_ref, c_ref, sems, wide, peaks):
    copies = [
        pltpu.make_async_copy(source, target, sems.at[k])
        for k, (source, target) in enumerate((
            (raw_hbm, raw_ref), (dlog_hbm, dlog_ref), (bias_hbm, bias_ref), (b_hbm, b_ref),
            (x_hbm, x_ref), (c_hbm, c_ref), (g_hbm, g_ref),
        ))
    ]
    for copy in copies:
        copy.start()
    for copy in copies[:3]:
        copy.wait()
    peaks[0:8] = jnp.zeros((8, 128), F32)
    peaks[0:1, :H] = jnp.exp(dlog_ref[...])
    peaks[1:2, :H] = bias_ref[...]
    heads = jnp.concatenate([peaks[0:8], jnp.zeros((120, 128), F32)], axis=0).T[:H]
    v = raw_ref[...].astype(F32) + heads[:, 1:2]
    dt = jnp.maximum(v, 0.0) + jnp.log1p(jnp.exp(-jnp.abs(v)))
    la = -heads[:, 0:1] * dt
    fin_ref[0] = dt
    fin_ref[1] = 1.0 / (1.0 + jnp.exp(-v))
    fin_ref[2] = la
    until = (iota((T, T), 0) <= iota((T, T), 1)).astype(BF16)
    run = summed_by(la, until) * LOG2E
    row_ref[...] = run
    total = run[:, T - 1 : T]
    wide[0:H] = run - jnp.log2(dt)
    wide[H : 2 * H] = jnp.exp2(total - run) * dt
    wide[2 * H : 3 * H] = jnp.exp2(run)
    wide[3 * H :] = jnp.zeros((128 - 3 * H, T), F32)
    columns = wide[...].T
    for i in range(STEPS):
        for part in range(3):
            at = H * part + 8 * i
            col_ref[i, :, 8 * part : 8 * part + 8] = columns[:, at : at + 8]
    keep = columns[T - 1 : T, 2 * H : 3 * H]
    keep_a = keep.astype(BF16).astype(F32)
    keep_b = (keep - keep_a).astype(BF16).astype(F32)
    keep_c = keep - keep_a - keep_b
    ext_ref[...] = jnp.zeros_like(ext_ref)
    ext_ref[0:1, :H] = keep_a
    ext_ref[1:2, :H] = keep_b * 512.0
    ext_ref[2:3, :H] = keep_c * 262144.0
    peaks[...] = jnp.zeros_like(peaks)
    for r, (source, start, maps) in enumerate(((x_ref, H, b_ref), (g_ref, 2 * H, c_ref))):
        copies[3 + 2 * r].wait()
        copies[4 + 2 * r].wait()
        left = maps[...].astype(F32).T.astype(BF16)
        for j in range(HP // 256):
            lanes = slice(256 * j, 256 * j + 256)
            weight = spread(columns, start + 4 * j, 4)
            high, low = halves(source[:, lanes].astype(F32) * weight)
            state = dot(left, high) + dot(left, low)
            most = jnp.max(jnp.abs(state), axis=0, keepdims=True)
            peaks[24 * r + 2 * j : 24 * r + 2 * j + 1] = most[:, :128]
            peaks[24 * r + 2 * j + 1 : 24 * r + 2 * j + 2] = most[:, 128:]
            for o in range(DEV):
                msg_ref[o, ROWS * r : ROWS * r + ROWS, lanes] = state[ROWS * o : ROWS * o + ROWS]
    lane = iota((24, 128), 1)
    pair = 2 * iota((24, 128), 0)
    for r in range(2):
        most = peaks[24 * r : 24 * r + 24]
        even = exponent(jnp.max(jnp.where(lane < 64, most, 0.0), axis=1, keepdims=True))
        odd = exponent(jnp.max(jnp.where(lane < 64, 0.0, most), axis=1, keepdims=True))
        placed = jnp.where(lane == pair, even, jnp.where(lane == pair + 1, odd, 0.0))
        ext_ref[3 + r : 4 + r] = jnp.sum(placed, axis=0, keepdims=True)
        scale = jnp.exp2(-jnp.where(lane < 64, even, odd))
        for j in range(HP // 128):
            scale_ref[r : r + 1, 128 * j : 128 * j + 128] = scale[j : j + 1]


def scan(got_ref, extra_ref, out_ref, ext_ref, wide):
    extra = [extra_ref[j] for j in range(DEV)]
    keep = [e[0:1] + e[1:2] * (1.0 / 512.0) + e[2:3] * (1.0 / 262144.0) for e in extra]
    in_s = [jnp.exp2(e[3:4]) for e in extra]
    in_g = [jnp.exp2(e[4:5]) for e in extra]
    top = 2.0**TOP
    zero = jnp.zeros((1, 128), F32)
    bound_s, bound_g = [zero], [zero]
    for k in range(DEV - 1):
        bound_s.append(keep[k] * bound_s[-1] + in_s[k] * top)
        back = DEV - 1 - k
        bound_g.append(keep[back] * bound_g[-1] + in_g[back] * top)
    bound_g = bound_g[::-1]
    exp_s = [exponent(b) for b in bound_s]
    exp_g = [exponent(b) for b in bound_g]
    for k in range(DEV):
        ext_ref[k, 0:1] = exp_s[k]
        ext_ref[k, 1:2] = exp_g[k]
        ext_ref[k, 2:8] = jnp.zeros((6, 128), F32)
    rows = keep + in_s + in_g + [jnp.exp2(-e) for e in exp_s] + [jnp.exp2(-e) for e in exp_g]
    rows = jnp.concatenate(rows, axis=0)
    parts = in_three(rows)
    count = 5 * DEV
    for c in range(STEPS):
        lanes = slice(STEP * c, STEP * c + STEP)
        hot = (iota((128, STEP), 0) == (iota((128, STEP), 1) + STEP * c) // 64).astype(BF16)
        over = dot(parts, hot)
        wide[:, lanes] = over[:count] + over[count : 2 * count] + over[2 * count :]
    for c in range(STEPS):
        lanes = slice(STEP * c, STEP * c + STEP)
        for first, scale, out, order in (
            (0, DEV, 3 * DEV, range(DEV)),
            (ROWS, 2 * DEV, 4 * DEV, range(DEV - 1, -1, -1)),
        ):
            held = jnp.zeros((ROWS, STEP), F32)
            for k in order:
                here = slice(first, first + ROWS)
                out_ref[k, here, lanes] = held * wide[out + k : out + k + 1, lanes]
                held = (
                    wide[k : k + 1, lanes] * held
                    + wide[scale + k : scale + k + 1, lanes] * got_ref[k, here, lanes]
                )


def inside(x_ref, g_ref, b_ref, c_ref, col_ref, row_ref,
           dx_ref, qrow_ref, qcol_ref, gx_ref, db_ref, dc_ref, score, total, qcol):
    i = pl.program_id(0)
    half = T // 2

    @pl.when(i == 0)
    def _():
        score[...] = dot_nt(b_ref[...], c_ref[...])
        total[...] = jnp.zeros_like(total)
        qcol[...] = jnp.zeros_like(qcol)

    causal = iota((half, T), 1) >= iota((half, T), 0)
    causal_end = iota((half, half), 1) >= iota((half, half), 0)
    lane = iota((half, 128), 1)
    for p in range(STEP // 128):
        lanes = slice(128 * p, 128 * p + 128)
        x = x_ref[:, lanes]
        g = g_ref[:, lanes]
        gx = jnp.sum(x.astype(F32) * g.astype(F32), axis=0, keepdims=True)
        gx_ref[:, lanes] = gx
        grads = []
        for q in range(2):
            k = 2 * p + q
            mine = iota((T, 128), 1) < 64 if q == 0 else iota((T, 128), 1) >= 64
            own = jnp.where(mine, x, jnp.zeros_like(x))
            at = 8 * i + k
            parts = []
            sums = []
            for start, width, keep in ((0, T, causal), (half, half, causal_end)):
                here = slice(start, start + half)
                later = slice(T - width, T)
                gap = row_ref[k : k + 1, later] - col_ref[0, here, k : k + 1]
                decay = jnp.exp2(jnp.where(keep, gap, -1e5))
                cross = dot_nt(own[here], g[later])
                weight = decay * score[here, later]
                high, low = halves(weight)
                parts.append(dot(high, g[later]) + dot(low, g[later]))
                total[here, later] += decay * cross
                pair = weight * cross
                sums.append(jnp.sum(pair, axis=0, keepdims=True))
                qcol[here] += jnp.where(lane == at, jnp.sum(pair, axis=1, keepdims=True), 0.0)
            qrow_ref[k : k + 1, :half] = sums[0][:, :half]
            qrow_ref[k : k + 1, half:] = sums[0][:, half:] + sums[1]
            grads.append(parts)
        for s in range(2):
            dx_ref[half * s : half * s + half, lanes] = jnp.where(
                lane < 64, grads[0][s], grads[1][s]
            )

    @pl.when(i == STEPS - 1)
    def _():
        high, low = halves(total[...])
        db_ref[...] = dot(high, c_ref[...]) + dot(low, c_ref[...])
        high, low = halves(total[...].T)
        dc_ref[...] = dot(high, b_ref[...]) + dot(low, b_ref[...])
        qcol_ref[...] = qcol[...].T[:H]


def entering(got_ref, first, i):
    lanes = slice(STEP * i, STEP * i + STEP)
    return jnp.concatenate([got_ref[o, first : first + ROWS, lanes] for o in range(DEV)], axis=0)


def twice(rows):
    return jnp.concatenate([rows, rows], axis=1)


def stacked(value):
    return jnp.concatenate(halves(value), axis=0)


def outside(x_hbm, g_hbm, b_ref, c_ref, col_ref, got_ref, all_ref, qrow_ref, qcol_ref, gx_ref,
            fin_ref, keep_ref, steps_ref, par_ref, x_ref, g_ref, sems, far_row, far_col):
    copies = [
        pltpu.make_async_copy(x_hbm, x_ref, sems.at[0]),
        pltpu.make_async_copy(g_hbm, g_ref, sems.at[1]),
    ]
    for copy in copies:
        copy.start()
    lane_sums = jnp.zeros((16, 128), F32)
    b_two, c_two = twice(b_ref[...]), twice(c_ref[...])
    for i in range(STEPS):
        whole = slice(STEP * i, STEP * i + STEP)
        state, slope = entering(got_ref, 0, i), entering(got_ref, ROWS, i)
        seen = dot(c_two, stacked(state))
        back = dot(b_two, stacked(slope))
        at = slice(8 * i, 8 * i + 8)
        into = col_ref[i, :, 8:16] * jnp.exp2(all_ref[1:2, at])
        outof = col_ref[i, :, 16:24] * jnp.exp2(all_ref[0:1, at])
        hot = (iota((STEP, 128), 1) == iota((STEP, 128), 0) // 64 + 8 * i).astype(BF16)
        both = jnp.concatenate(
            [jnp.sum(state * slope, axis=0, keepdims=True), gx_ref[:, whole],
             jnp.zeros((14, STEP), F32)],
            axis=0,
        )
        if i == 0:
            for copy in copies:
                copy.wait()
        rows = spread(outof, 0, 8) * g_ref[:, whole].astype(F32) * seen
        cols = spread(into, 0, 8) * x_ref[:, whole].astype(F32) * back
        out = dot(jnp.concatenate([stacked(rows), stacked(cols), in_three(both)], axis=0), hot)
        rows = out[0:T] + out[T : 2 * T]
        cols = out[2 * T : 3 * T] + out[3 * T : 4 * T]
        far_row[...] = rows if i == 0 else far_row[...] + rows
        far_col[...] = cols if i == 0 else far_col[...] + cols
        lane_sums += out[4 * T : 4 * T + 16] + out[4 * T + 16 : 4 * T + 32] + out[4 * T + 32 :]
    dt, gate, la = fin_ref[0], fin_ref[1], fin_ref[2]
    rows, cols = far_row[...].T[:H], far_col[...].T[:H]
    since = (iota((T, T), 0) >= iota((T, T), 1)).astype(BF16)
    before = (iota((T, T), 0) < iota((T, T), 1)).astype(BF16)
    summed = summed_by(qrow_ref[...] - qcol_ref[...] + rows, since) + summed_by(cols, before)
    keep = keep_ref[0:1] + keep_ref[1:2] * (1.0 / 512.0) + keep_ref[2:3] * (1.0 / 262144.0)
    ends = keep * jnp.exp2(all_ref[0:1]) * lane_sums[0:1] * jnp.exp2(all_ref[1:2])
    ends = jnp.concatenate([ends, jnp.zeros((127, 128), F32)], axis=0).T[:H, 0:1]
    rate = la * (summed + ends)
    grad = gate * ((qcol_ref[...] + cols + rate) / dt)
    steps_ref[...] = grad
    sums = dot_nt(jnp.ones((8, T), BF16), in_three(jnp.concatenate([rate, grad], axis=0)))[0:1]
    sums = sums[:, : 2 * H] + sums[:, 2 * H : 4 * H] + sums[:, 4 * H :]
    mine = jnp.concatenate(
        [sums[:, :H], lane_sums[1:2, :H], sums[:, H:], jnp.zeros((1, 128 - 3 * H), F32)], axis=1
    )
    par_ref[...] = jnp.broadcast_to(mine[None], par_ref.shape)


def maps(x_hbm, g_hbm, b_hbm, col_hbm, db_hbm, dc_hbm, near_hbm, got_ref, all_ref, skip_ref,
         dx_hbm, db_ref, dc_ref, x_ref, g_ref, b_ref, col_ref, near_ref, part_ref, dx_ref, sems):
    copies = [
        pltpu.make_async_copy(source, target, sems.at[k])
        for k, (source, target) in enumerate((
            (col_hbm, col_ref), (b_hbm, b_ref), (x_hbm, x_ref), (db_hbm, db_ref),
            (g_hbm, g_ref), (dc_hbm, dc_ref), (near_hbm, near_ref),
        ))
    ]
    leave = pltpu.make_async_copy(dx_ref, dx_hbm, sems.at[len(copies)])
    for copy in copies:
        copy.start()
    for copy in copies[:4]:
        copy.wait()
    b_two = twice(b_ref[...])
    first = iota((1, 128), 1) < 64

    def gained(rows, weight, other):
        out = dot_nt(stacked(weight * rows), stacked(other))
        return out[:T, :N] + out[:T, N:] + out[T:, :N]

    for i in range(STEPS):
        whole = slice(STEP * i, STEP * i + STEP)
        at = slice(8 * i, 8 * i + 8)
        into = spread(col_ref[i, :, 8:16] * jnp.exp2(all_ref[1:2, at]), 0, 8)
        slope = entering(got_ref, ROWS, i)
        part_ref[:, whole] = into * dot(b_two, stacked(slope))
        db_ref[...] += gained(x_ref[:, whole].astype(F32), into, slope)
    for copy in copies[4:]:
        copy.wait()
    for i in range(STEPS):
        whole = slice(STEP * i, STEP * i + STEP)
        g = g_ref[:, whole].astype(F32)
        skip = jnp.concatenate(
            [jnp.where(first, skip_ref[k], skip_ref[k + 1]) for k in range(8 * i, 8 * i + 8, 2)],
            axis=1,
        )
        dx_ref[:, whole] = (near_ref[:, whole] + part_ref[:, whole] + skip * g).astype(BF16)
    leave.start()
    for i in range(STEPS):
        at = slice(8 * i, 8 * i + 8)
        outof = spread(col_ref[i, :, 16:24] * jnp.exp2(all_ref[0:1, at]), 0, 8)
        g = g_ref[:, STEP * i : STEP * i + STEP].astype(F32)
        dc_ref[...] += gained(g, outof, entering(got_ref, 0, i))
    leave.wait()


def spec(shape, index=None):
    index = index or (lambda i: (0,) * len(shape))
    return pl.BlockSpec(shape, index)


def shape(*dims, dtype=F32):
    return jax.ShapeDtypeStruct(dims, dtype)


def coded(body):
    return (body * jnp.abs(body)).astype(jnp.float16)


def decoded(body):
    body = body.astype(F32)
    return near(body * lax.rsqrt(jnp.maximum(jnp.abs(body), TINY)))


def near(array):
    return pltpu.with_memory_space_constraint(array, pltpu.VMEM)


def far_off(*arrays):
    return [pltpu.with_memory_space_constraint(a, pltpu.HBM) for a in arrays]


def exchange(message):
    return lax.all_to_all(message, SEQ, 0, 0, tiled=True)


def on_device(
    tokens_in, step_raw, input_map, output_map, decay_log, skip_gain, step_bias, grad_out
):
    x, raw, b, c, g = (m[0] for m in (tokens_in, step_raw, input_map, output_map, grad_out))
    ranks = lax.axis_size(SEQ) * lax.axis_size(DP)
    factor = 1.0 / math.sqrt(ranks * T * (HP // H))
    vmem = pl.BlockSpec(memory_space=pltpu.VMEM)
    cost = pl.CostEstimate(
        flops=4_000_000_000, bytes_accessed=8_000_000, transcendentals=2_000_000
    )
    room = pltpu.CompilerParams(vmem_limit_bytes=24 * 1024 * 1024)
    msg, scale, ext, cols, rows, fin = pl.pallas_call(
        prepare,
        in_specs=(pl.BlockSpec(memory_space=pltpu.HBM),) * 7,
        out_shape=(
            pltpu.VMEM((DEV, 2 * ROWS, HP), F32), pltpu.VMEM((2, HP), F32),
            pltpu.VMEM((8, 128), F32), pltpu.HBM((STEPS, T, 24), F32), pltpu.HBM((H, T), F32),
            pltpu.HBM((3, H, T), F32),
        ),
        out_specs=(vmem,) * 6,
        scratch_shapes=[
            pltpu.VMEM((H, T), BF16), pltpu.VMEM((1, H), F32), pltpu.VMEM((1, H), F32),
            pltpu.VMEM((T, HP), BF16), pltpu.VMEM((T, HP), BF16), pltpu.VMEM((T, N), BF16),
            pltpu.VMEM((T, N), BF16), pltpu.SemaphoreType.DMA((7,)),
            pltpu.VMEM((128, T), F32), pltpu.VMEM((48, 128), F32),
        ],
        compiler_params=room,
        name="prepare",
    )(*far_off(raw.T, decay_log[None], step_bias[None], x, g, b, c))
    scale = jnp.broadcast_to(scale[:, None], (2, ROWS, HP)).reshape(2 * ROWS, HP)
    extra = jnp.pad(ext, ((0, 2 * ROWS - 8), (0, 0))).astype(jnp.float16)
    extra = jnp.broadcast_to(extra[None], (DEV, 2 * ROWS, 128))
    got = exchange(jnp.concatenate([coded(msg * scale[None]), extra], axis=2))
    got, got_ext = decoded(got[:, :, :HP]), got[:, 0:8, HP:].astype(F32)

    lanes = spec((T, STEP), lambda i: (0, i))
    full = spec((T, N))
    heads = spec((H, T))
    cols_spec = spec((1, T, 24), lambda i: (i, 0, 0))
    gx_spec = spec((1, STEP), lambda i: (0, i))
    near_dx, qrow, qcol, gx, db, dc = pl.pallas_call(
        inside,
        grid=(STEPS,),
        in_specs=[lanes, lanes, full, full, cols_spec, spec((8, T), lambda i: (i, 0))],
        out_specs=[lanes, spec((8, T), lambda i: (i, 0)), heads, gx_spec, full, full],
        out_shape=(
            pltpu.HBM((T, HP), F32), pltpu.HBM((H, T), F32), pltpu.HBM((H, T), F32),
            pltpu.HBM((1, HP), F32), pltpu.HBM((T, N), F32), pltpu.HBM((T, N), F32),
        ),
        scratch_shapes=[
            pltpu.VMEM((T, T), F32), pltpu.VMEM((T, T), F32), pltpu.VMEM((T, 128), F32),
        ],
        cost_estimate=cost,
        compiler_params=room,
        name="inside",
    )(x, g, b, c, cols, rows)

    sent, sent_ext = pl.pallas_call(
        scan,
        in_specs=(vmem, vmem),
        out_shape=(pltpu.VMEM((DEV, 2 * ROWS, HP), F32), pltpu.VMEM((DEV, 8, 128), F32)),
        out_specs=(vmem, vmem),
        scratch_shapes=[pltpu.VMEM((5 * DEV, HP), F32)],
        compiler_params=room,
        name="scan",
    )(got, got_ext)
    back = decoded(exchange(coded(sent)))
    scales = lax.dynamic_index_in_dim(sent_ext, lax.axis_index(SEQ), 0, keepdims=False)

    hbm = pl.BlockSpec(memory_space=pltpu.HBM)
    smem = pl.BlockSpec(memory_space=pltpu.SMEM)
    steps, everyone = pl.pallas_call(
        outside,
        in_specs=[hbm] * 2 + [vmem] * 10,
        out_specs=[vmem] * 2,
        out_shape=(shape(H, T), shape(ranks, 1, 128)),
        scratch_shapes=[
            pltpu.VMEM((T, HP), BF16), pltpu.VMEM((T, HP), BF16), pltpu.SemaphoreType.DMA((2,)),
            pltpu.VMEM((T, 128), F32), pltpu.VMEM((T, 128), F32),
        ],
        compiler_params=room,
        name="outside",
    )(*far_off(x, g), near(b), near(c), near(cols), back, near(scales), near(qrow), near(qcol),
      near(gx), near(fin), near(ext))
    everyone = lax.all_to_all(everyone, SEQ_DP, 0, 0, tiled=True)
    dx, db, dc = pl.pallas_call(
        maps,
        in_specs=[hbm] * 7 + [vmem] * 2 + [smem],
        out_specs=[hbm, vmem, vmem],
        out_shape=(pltpu.HBM((T, HP), BF16), shape(T, N), shape(T, N)),
        scratch_shapes=[
            pltpu.VMEM((T, HP), BF16), pltpu.VMEM((T, HP), BF16), pltpu.VMEM((T, N), BF16),
            pltpu.VMEM((STEPS, T, 24), F32), pltpu.VMEM((T, HP), F32), pltpu.VMEM((T, HP), F32),
            pltpu.VMEM((T, HP), BF16), pltpu.SemaphoreType.DMA((8,)),
        ],
        cost_estimate=cost,
        compiler_params=room,
        name="maps",
    )(*far_off(x, g, b, cols, db, dc, near_dx), back, near(scales), skip_gain)
    total = jnp.sum(everyone, axis=(0, 1)) * factor
    return (
        dx[None], steps.T[None], db[None], dc[None],
        total[:H], total[H : 2 * H], total[2 * H : 3 * H],
    )


def build(split):
    held = P(DP, SEQ, None)
    return jax.shard_map(
        on_device,
        mesh=split,
        in_specs=(held, held, held, held, P(), P(), P(), held),
        out_specs=(held, held, held, held, P(), P(), P()),
        check_vma=False,
    )


def solution(mesh):
    return build(Mesh(mesh.devices.reshape(2, 4, 2, 8, 2), SEQ_DP))
```

```python
import functools
import math

import jax
import jax.numpy as jnp
from jax import lax
from jax.experimental import pallas as pl
from jax.experimental.pallas import tpu as pltpu
from jax.sharding import Mesh
from jax.sharding import PartitionSpec as P

SEQ = ("seq_0", "seq_1")
DP = ("dp_0", "dp_1", "dp_2")
SEQ_DP = ("seq_0", "seq_1", "dp_0", "dp_1", "dp_2")

F32 = jnp.float32
BF16 = jnp.bfloat16
LOG2E = math.log2(math.e)
T = 256
H = 40
HP = 2560
N = 128
DEV = 8
ROWS = N // DEV
STEP = 512
STEPS = HP // STEP
TOP = 7.0
TINY = 1e-30


def halves(value):
    high = value.astype(BF16)
    return high, (value - high.astype(F32)).astype(BF16)


def dot(a, b):
    return jnp.dot(a, b, preferred_element_type=F32)


def dot_nt(a, b):
    return lax.dot_general(a, b, (((1,), (1,)), ((), ())), preferred_element_type=F32)


def in_three(value):
    high = value.astype(BF16).astype(F32)
    mid = (value - high).astype(BF16).astype(F32)
    return jnp.concatenate([high, mid, value - high - mid], axis=0).astype(BF16)


def summed_by(value, zero_one):
    out = dot(in_three(value), zero_one)
    n = value.shape[0]
    return out[:n] + out[n : 2 * n] + out[2 * n :]


def iota(shape, dim):
    return lax.broadcasted_iota(jnp.int32, shape, dim)


def spread(columns, k, count):
    first = iota((T, 128), 1) < 64
    pairs = [
        jnp.where(first, columns[:, j : j + 1], columns[:, j + 1 : j + 2])
        for j in range(k, k + count, 2)
    ]
    return jnp.concatenate(pairs, axis=1)


def exponent(bound):
    return jnp.ceil(jnp.log2(bound + TINY)) - TOP


def prepare(raw_hbm, dlog_hbm, bias_hbm, x_hbm, g_hbm, b_hbm, c_hbm,
            msg_ref, scale_ref, ext_ref, col_ref, row_ref, fin_ref,
            raw_ref, dlog_ref, bias_ref, x_ref, g_ref, b_ref, c_ref, sems, wide, peaks):
    copies = [
        pltpu.make_async_copy(source, target, sems.at[k])
        for k, (source, target) in enumerate((
            (raw_hbm, raw_ref), (dlog_hbm, dlog_ref), (bias_hbm, bias_ref), (b_hbm, b_ref),
            (x_hbm, x_ref), (c_hbm, c_ref), (g_hbm, g_ref),
        ))
    ]
    for copy in copies:
        copy.start()
    for copy in copies[:3]:
        copy.wait()
    peaks[0:8] = jnp.zeros((8, 128), F32)
    peaks[0:1, :H] = jnp.exp(dlog_ref[...])
    peaks[1:2, :H] = bias_ref[...]
    heads = jnp.concatenate([peaks[0:8], jnp.zeros((120, 128), F32)], axis=0).T[:H]
    v = raw_ref[...].astype(F32) + heads[:, 1:2]
    dt = jnp.maximum(v, 0.0) + jnp.log1p(jnp.exp(-jnp.abs(v)))
    la = -heads[:, 0:1] * dt
    fin_ref[0] = dt
    fin_ref[1] = 1.0 / (1.0 + jnp.exp(-v))
    fin_ref[2] = la
    until = (iota((T, T), 0) <= iota((T, T), 1)).astype(BF16)
    run = summed_by(la, until) * LOG2E
    row_ref[...] = run
    total = run[:, T - 1 : T]
    wide[0:H] = run - jnp.log2(dt)
    wide[H : 2 * H] = fin_ref[3] = jnp.exp2(total - run) * dt
    wide[2 * H : 3 * H] = fin_ref[4] = jnp.exp2(run)
    wide[3 * H :] = jnp.zeros((128 - 3 * H, T), F32)
    columns = wide[...].T
    for i in range(STEPS):
        for part in range(3):
            at = H * part + 8 * i
            col_ref[i, :, 8 * part : 8 * part + 8] = columns[:, at : at + 8]
    keep = columns[T - 1 : T, 2 * H : 3 * H]
    keep_a = keep.astype(BF16).astype(F32)
    keep_b = (keep - keep_a).astype(BF16).astype(F32)
    keep_c = keep - keep_a - keep_b
    ext_ref[...] = jnp.zeros_like(ext_ref)
    ext_ref[0:1, :H] = keep_a
    ext_ref[1:2, :H] = keep_b * 512.0
    ext_ref[2:3, :H] = keep_c * 262144.0
    peaks[...] = jnp.zeros_like(peaks)
    for r, (source, start, maps) in enumerate(((x_ref, H, b_ref), (g_ref, 2 * H, c_ref))):
        copies[3 + 2 * r].wait()
        copies[4 + 2 * r].wait()
        left = maps[...].astype(F32).T.astype(BF16)
        for j in range(HP // 256):
            lanes = slice(256 * j, 256 * j + 256)
            weight = spread(columns, start + 4 * j, 4)
            high, low = halves(source[:, lanes].astype(F32) * weight)
            state = dot(left, high) + dot(left, low)
            most = jnp.max(jnp.abs(state), axis=0, keepdims=True)
            peaks[24 * r + 2 * j : 24 * r + 2 * j + 1] = most[:, :128]
            peaks[24 * r + 2 * j + 1 : 24 * r + 2 * j + 2] = most[:, 128:]
            for o in range(DEV):
                msg_ref[o, ROWS * r : ROWS * r + ROWS, lanes] = state[ROWS * o : ROWS * o + ROWS]
    lane = iota((24, 128), 1)
    pair = 2 * iota((24, 128), 0)
    for r in range(2):
        most = peaks[24 * r : 24 * r + 24]
        even = exponent(jnp.max(jnp.where(lane < 64, most, 0.0), axis=1, keepdims=True))
        odd = exponent(jnp.max(jnp.where(lane < 64, 0.0, most), axis=1, keepdims=True))
        placed = jnp.where(lane == pair, even, jnp.where(lane == pair + 1, odd, 0.0))
        ext_ref[3 + r : 4 + r] = jnp.sum(placed, axis=0, keepdims=True)
        scale = jnp.exp2(-jnp.where(lane < 64, even, odd))
        for j in range(HP // 128):
            scale_ref[r : r + 1, 128 * j : 128 * j + 128] = scale[j : j + 1]


def scan(got_ref, extra_ref, out_ref, ext_ref, wide):
    extra = [extra_ref[j] for j in range(DEV)]
    keep = [e[0:1] + e[1:2] * (1.0 / 512.0) + e[2:3] * (1.0 / 262144.0) for e in extra]
    in_s = [jnp.exp2(e[3:4]) for e in extra]
    in_g = [jnp.exp2(e[4:5]) for e in extra]
    top = 2.0**TOP
    zero = jnp.zeros((1, 128), F32)
    bound_s, bound_g = [zero], [zero]
    for k in range(DEV - 1):
        bound_s.append(keep[k] * bound_s[-1] + in_s[k] * top)
        back = DEV - 1 - k
        bound_g.append(keep[back] * bound_g[-1] + in_g[back] * top)
    bound_g = bound_g[::-1]
    exp_s = [exponent(b) for b in bound_s]
    exp_g = [exponent(b) for b in bound_g]
    for k in range(DEV):
        ext_ref[k, 0:1] = exp_s[k]
        ext_ref[k, 1:2] = exp_g[k]
        ext_ref[k, 2:8] = jnp.zeros((6, 128), F32)
    rows = keep + in_s + in_g + [jnp.exp2(-e) for e in exp_s] + [jnp.exp2(-e) for e in exp_g]
    rows = jnp.concatenate(rows, axis=0)
    parts = in_three(rows)
    count = 5 * DEV
    for c in range(STEPS):
        lanes = slice(STEP * c, STEP * c + STEP)
        hot = (iota((128, STEP), 0) == (iota((128, STEP), 1) + STEP * c) // 64).astype(BF16)
        over = dot(parts, hot)
        wide[:, lanes] = over[:count] + over[count : 2 * count] + over[2 * count :]
    for c in range(STEPS):
        lanes = slice(STEP * c, STEP * c + STEP)
        for first, scale, out, order in (
            (0, DEV, 3 * DEV, range(DEV)),
            (ROWS, 2 * DEV, 4 * DEV, range(DEV - 1, -1, -1)),
        ):
            held = jnp.zeros((ROWS, STEP), F32)
            for k in order:
                here = slice(first, first + ROWS)
                out_ref[k, here, lanes] = held * wide[out + k : out + k + 1, lanes]
                held = (
                    wide[k : k + 1, lanes] * held
                    + wide[scale + k : scale + k + 1, lanes] * got_ref[k, here, lanes]
                )


def inside(x_ref, g_ref, b_ref, c_ref, col_ref, row_ref,
           dx_ref, qrow_ref, qcol_ref, gx_ref, db_ref, dc_ref, score, total, qcol):
    i = pl.program_id(0)
    half = T // 2

    @pl.when(i == 0)
    def _():
        score[...] = dot_nt(b_ref[...], c_ref[...])
        total[...] = jnp.zeros_like(total)
        qcol[...] = jnp.zeros_like(qcol)

    causal = iota((half, T), 1) >= iota((half, T), 0)
    causal_end = iota((half, half), 1) >= iota((half, half), 0)
    lane = iota((half, 128), 1)
    for p in range(STEP // 128):
        lanes = slice(128 * p, 128 * p + 128)
        x = x_ref[:, lanes]
        g = g_ref[:, lanes]
        gx = jnp.sum(x.astype(F32) * g.astype(F32), axis=0, keepdims=True)
        gx_ref[:, lanes] = gx
        grads = []
        for q in range(2):
            k = 2 * p + q
            mine = iota((T, 128), 1) < 64 if q == 0 else iota((T, 128), 1) >= 64
            own = jnp.where(mine, x, jnp.zeros_like(x))
            at = 8 * i + k
            parts = []
            sums = []
            for start, width, keep in ((0, T, causal), (half, half, causal_end)):
                here = slice(start, start + half)
                later = slice(T - width, T)
                gap = row_ref[k : k + 1, later] - col_ref[0, here, k : k + 1]
                decay = jnp.exp2(jnp.where(keep, gap, -1e5))
                cross = dot_nt(own[here], g[later])
                weight = decay * score[here, later]
                high, low = halves(weight)
                parts.append(dot(high, g[later]) + dot(low, g[later]))
                total[here, later] += decay * cross
                pair = weight * cross
                sums.append(jnp.sum(pair, axis=0, keepdims=True))
                qcol[here] += jnp.where(lane == at, jnp.sum(pair, axis=1, keepdims=True), 0.0)
            qrow_ref[k : k + 1, :half] = sums[0][:, :half]
            qrow_ref[k : k + 1, half:] = sums[0][:, half:] + sums[1]
            grads.append(parts)
        for s in range(2):
            dx_ref[half * s : half * s + half, lanes] = jnp.where(
                lane < 64, grads[0][s], grads[1][s]
            )

    @pl.when(i == STEPS - 1)
    def _():
        high, low = halves(total[...])
        db_ref[...] = dot(high, c_ref[...]) + dot(low, c_ref[...])
        high, low = halves(total[...].T)
        dc_ref[...] = dot(high, b_ref[...]) + dot(low, b_ref[...])
        qcol_ref[...] = qcol[...].T[:H]


def entering(got_ref, first, i):
    lanes = slice(STEP * i, STEP * i + STEP)
    return jnp.concatenate([got_ref[o, first : first + ROWS, lanes] for o in range(DEV)], axis=0)


def twice(rows):
    return jnp.concatenate([rows, rows], axis=1)


def stacked(value):
    return jnp.concatenate(halves(value), axis=0)


def outside(x_hbm, g_hbm, b_ref, c_ref, got_ref, all_ref, qrow_ref, qcol_ref, gx_ref,
            fin_ref, keep_ref, steps_ref, par_ref, x_ref, g_ref, sems, far_row, far_col):
    copies = [
        pltpu.make_async_copy(x_hbm, x_ref, sems.at[0]),
        pltpu.make_async_copy(g_hbm, g_ref, sems.at[1]),
    ]
    for copy in copies:
        copy.start()
    lane_sums = jnp.zeros((16, 128), F32)
    b_two, c_two = twice(b_ref[...]), twice(c_ref[...])
    lane = iota((T, 128), 1)
    far_col[...] = jnp.zeros_like(far_col)
    for i in range(STEPS):
        whole = slice(STEP * i, STEP * i + STEP)
        state, slope = entering(got_ref, 0, i), entering(got_ref, ROWS, i)
        seen = dot(c_two, stacked(state))
        back = dot(b_two, stacked(slope))
        hot = (iota((STEP, 128), 1) == iota((STEP, 128), 0) // 64 + 8 * i).astype(BF16)
        both = jnp.concatenate(
            [jnp.sum(state * slope, axis=0, keepdims=True), gx_ref[:, whole],
             jnp.zeros((14, STEP), F32)],
            axis=0,
        )
        if i == 0:
            for copy in copies:
                copy.wait()
        rows = g_ref[:, whole].astype(F32) * seen
        cols = x_ref[:, whole].astype(F32) * back
        out = dot(jnp.concatenate([stacked(rows), in_three(both)], axis=0), hot)
        rows = out[0:T] + out[T : 2 * T]
        far_row[...] = rows if i == 0 else far_row[...] + rows
        held = far_col[...]
        for p in range(STEP // 128):
            part = cols[:, 128 * p : 128 * p + 128]
            even = jnp.sum(jnp.where(lane < 64, part, 0.0), axis=1, keepdims=True)
            odd = jnp.sum(jnp.where(lane < 64, 0.0, part), axis=1, keepdims=True)
            at = 8 * i + 2 * p
            held = jnp.where(lane == at, even, jnp.where(lane == at + 1, odd, held))
        far_col[...] = held
        last = out[2 * T :]
        lane_sums += last[0:16] + last[16:32] + last[32:48]
    dt, gate, la = fin_ref[0], fin_ref[1], fin_ref[2]
    keep = keep_ref[0:1] + keep_ref[1:2] * (1.0 / 512.0) + keep_ref[2:3] * (1.0 / 262144.0)
    scale_s, scale_g = jnp.exp2(all_ref[0:1]), jnp.exp2(all_ref[1:2])
    ends = keep * scale_s * lane_sums[0:1] * scale_g
    by_head = jnp.concatenate([ends, scale_s, scale_g, jnp.zeros((125, 128), F32)], axis=0).T[:H]
    rows = far_row[...].T[:H] * (fin_ref[4] * by_head[:, 1:2])
    cols = far_col[...].T[:H] * (fin_ref[3] * by_head[:, 2:3])
    since = (iota((T, T), 0) >= iota((T, T), 1)).astype(BF16)
    before = (iota((T, T), 0) < iota((T, T), 1)).astype(BF16)
    summed = summed_by(qrow_ref[...] - qcol_ref[...] + rows, since) + summed_by(cols, before)
    rate = la * (summed + by_head[:, 0:1])
    grad = gate * ((qcol_ref[...] + cols + rate) / dt)
    steps_ref[...] = grad
    sums = dot_nt(jnp.ones((8, T), BF16), in_three(jnp.concatenate([rate, grad], axis=0)))[0:1]
    sums = sums[:, : 2 * H] + sums[:, 2 * H : 4 * H] + sums[:, 4 * H :]
    mine = jnp.concatenate(
        [sums[:, :H], lane_sums[1:2, :H], sums[:, H:], jnp.zeros((1, 128 - 3 * H), F32)], axis=1
    )
    par_ref[...] = jnp.broadcast_to(mine[None], par_ref.shape)


def maps(x_hbm, g_hbm, b_hbm, col_hbm, db_hbm, dc_hbm, near_hbm, got_ref, all_ref, skip_ref,
         dx_hbm, db_ref, dc_ref, x_ref, g_ref, b_ref, col_ref, near_ref, part_ref, dx_ref, sems):
    copies = [
        pltpu.make_async_copy(source, target, sems.at[k])
        for k, (source, target) in enumerate((
            (col_hbm, col_ref), (b_hbm, b_ref), (x_hbm, x_ref), (db_hbm, db_ref),
            (g_hbm, g_ref), (dc_hbm, dc_ref), (near_hbm, near_ref),
        ))
    ]
    leave = pltpu.make_async_copy(dx_ref, dx_hbm, sems.at[len(copies)])
    for copy in copies:
        copy.start()
    for copy in copies[:4]:
        copy.wait()
    b_two = twice(b_ref[...])
    first = iota((1, 128), 1) < 64

    def gained(rows, weight, other):
        out = dot_nt(stacked(weight * rows), stacked(other))
        return out[:T, :N] + out[:T, N:] + out[T:, :N]

    for i in range(STEPS):
        whole = slice(STEP * i, STEP * i + STEP)
        at = slice(8 * i, 8 * i + 8)
        into = spread(col_ref[i, :, 8:16] * jnp.exp2(all_ref[1:2, at]), 0, 8)
        slope = entering(got_ref, ROWS, i)
        part_ref[:, whole] = into * dot(b_two, stacked(slope))
        db_ref[...] += gained(x_ref[:, whole].astype(F32), into, slope)
    for copy in copies[4:]:
        copy.wait()
    for i in range(STEPS):
        whole = slice(STEP * i, STEP * i + STEP)
        g = g_ref[:, whole].astype(F32)
        skip = jnp.concatenate(
            [jnp.where(first, skip_ref[k], skip_ref[k + 1]) for k in range(8 * i, 8 * i + 8, 2)],
            axis=1,
        )
        dx_ref[:, whole] = (near_ref[:, whole] + part_ref[:, whole] + skip * g).astype(BF16)
    leave.start()
    for i in range(STEPS):
        at = slice(8 * i, 8 * i + 8)
        outof = spread(col_ref[i, :, 16:24] * jnp.exp2(all_ref[0:1, at]), 0, 8)
        g = g_ref[:, STEP * i : STEP * i + STEP].astype(F32)
        dc_ref[...] += gained(g, outof, entering(got_ref, 0, i))
    leave.wait()


def spec(shape, index=None):
    index = index or (lambda i: (0,) * len(shape))
    return pl.BlockSpec(shape, index)


def shape(*dims, dtype=F32):
    return jax.ShapeDtypeStruct(dims, dtype)


def coded(body):
    return (body * jnp.abs(body)).astype(jnp.float16)


def decoded(body):
    body = body.astype(F32)
    return near(body * lax.rsqrt(jnp.maximum(jnp.abs(body), TINY)))


def near(array):
    return pltpu.with_memory_space_constraint(array, pltpu.VMEM)


def far_off(*arrays):
    return [pltpu.with_memory_space_constraint(a, pltpu.HBM) for a in arrays]


def exchange(message):
    return lax.all_to_all(message, SEQ, 0, 0, tiled=True)


def on_device(
    tokens_in, step_raw, input_map, output_map, decay_log, skip_gain, step_bias, grad_out
):
    x, raw, b, c, g = (m[0] for m in (tokens_in, step_raw, input_map, output_map, grad_out))
    ranks = lax.axis_size(SEQ) * lax.axis_size(DP)
    factor = 1.0 / math.sqrt(ranks * T * (HP // H))
    vmem = pl.BlockSpec(memory_space=pltpu.VMEM)
    cost = pl.CostEstimate(
        flops=4_000_000_000, bytes_accessed=8_000_000, transcendentals=2_000_000
    )
    room = pltpu.CompilerParams(vmem_limit_bytes=24 * 1024 * 1024)
    msg, scale, ext, cols, rows, fin = pl.pallas_call(
        prepare,
        in_specs=(pl.BlockSpec(memory_space=pltpu.HBM),) * 7,
        out_shape=(
            pltpu.VMEM((DEV, 2 * ROWS, HP), F32), pltpu.VMEM((2, HP), F32),
            pltpu.VMEM((8, 128), F32), pltpu.HBM((STEPS, T, 24), F32), pltpu.HBM((H, T), F32),
            pltpu.HBM((5, H, T), F32),
        ),
        out_specs=(vmem,) * 6,
        scratch_shapes=[
            pltpu.VMEM((H, T), BF16), pltpu.VMEM((1, H), F32), pltpu.VMEM((1, H), F32),
            pltpu.VMEM((T, HP), BF16), pltpu.VMEM((T, HP), BF16), pltpu.VMEM((T, N), BF16),
            pltpu.VMEM((T, N), BF16), pltpu.SemaphoreType.DMA((7,)),
            pltpu.VMEM((128, T), F32), pltpu.VMEM((48, 128), F32),
        ],
        compiler_params=room,
        name="prepare",
    )(*far_off(raw.T, decay_log[None], step_bias[None], x, g, b, c))
    scale = jnp.broadcast_to(scale[:, None], (2, ROWS, HP)).reshape(2 * ROWS, HP)
    extra = jnp.pad(ext, ((0, 2 * ROWS - 8), (0, 0))).astype(jnp.float16)
    extra = jnp.broadcast_to(extra[None], (DEV, 2 * ROWS, 128))
    got = exchange(jnp.concatenate([coded(msg * scale[None]), extra], axis=2))
    got, got_ext = decoded(got[:, :, :HP]), got[:, 0:8, HP:].astype(F32)

    lanes = spec((T, STEP), lambda i: (0, i))
    full = spec((T, N))
    heads = spec((H, T))
    cols_spec = spec((1, T, 24), lambda i: (i, 0, 0))
    gx_spec = spec((1, STEP), lambda i: (0, i))
    near_dx, qrow, qcol, gx, db, dc = pl.pallas_call(
        inside,
        grid=(STEPS,),
        in_specs=[lanes, lanes, full, full, cols_spec, spec((8, T), lambda i: (i, 0))],
        out_specs=[lanes, spec((8, T), lambda i: (i, 0)), heads, gx_spec, full, full],
        out_shape=(
            pltpu.HBM((T, HP), F32), pltpu.HBM((H, T), F32), pltpu.HBM((H, T), F32),
            pltpu.HBM((1, HP), F32), pltpu.HBM((T, N), F32), pltpu.HBM((T, N), F32),
        ),
        scratch_shapes=[
            pltpu.VMEM((T, T), F32), pltpu.VMEM((T, T), F32), pltpu.VMEM((T, 128), F32),
        ],
        cost_estimate=cost,
        compiler_params=room,
        name="inside",
    )(x, g, b, c, cols, rows)

    sent, sent_ext = pl.pallas_call(
        scan,
        in_specs=(vmem, vmem),
        out_shape=(pltpu.VMEM((DEV, 2 * ROWS, HP), F32), pltpu.VMEM((DEV, 8, 128), F32)),
        out_specs=(vmem, vmem),
        scratch_shapes=[pltpu.VMEM((5 * DEV, HP), F32)],
        compiler_params=room,
        name="scan",
    )(got, got_ext)
    back = decoded(exchange(coded(sent)))
    scales = lax.dynamic_index_in_dim(sent_ext, lax.axis_index(SEQ), 0, keepdims=False)

    hbm = pl.BlockSpec(memory_space=pltpu.HBM)
    smem = pl.BlockSpec(memory_space=pltpu.SMEM)
    steps, everyone = pl.pallas_call(
        outside,
        in_specs=[hbm] * 2 + [vmem] * 9,
        out_specs=[vmem] * 2,
        out_shape=(shape(H, T), shape(ranks, 1, 128)),
        scratch_shapes=[
            pltpu.VMEM((T, HP), BF16), pltpu.VMEM((T, HP), BF16), pltpu.SemaphoreType.DMA((2,)),
            pltpu.VMEM((T, 128), F32), pltpu.VMEM((T, 128), F32),
        ],
        compiler_params=room,
        name="outside",
    )(*far_off(x, g), near(b), near(c), back, near(scales), near(qrow), near(qcol),
      near(gx), near(fin), near(ext))
    everyone = lax.all_to_all(everyone, SEQ_DP, 0, 0, tiled=True)
    dx, db, dc = pl.pallas_call(
        maps,
        in_specs=[hbm] * 7 + [vmem] * 2 + [smem],
        out_specs=[hbm, vmem, vmem],
        out_shape=(pltpu.HBM((T, HP), BF16), shape(T, N), shape(T, N)),
        scratch_shapes=[
            pltpu.VMEM((T, HP), BF16), pltpu.VMEM((T, HP), BF16), pltpu.VMEM((T, N), BF16),
            pltpu.VMEM((STEPS, T, 24), F32), pltpu.VMEM((T, HP), F32), pltpu.VMEM((T, HP), F32),
            pltpu.VMEM((T, HP), BF16), pltpu.SemaphoreType.DMA((8,)),
        ],
        cost_estimate=cost,
        compiler_params=room,
        name="maps",
    )(*far_off(x, g, b, cols, db, dc, near_dx), back, near(scales), skip_gain)
    total = jnp.sum(everyone, axis=(0, 1)) * factor
    return (
        dx[None], steps.T[None], db[None], dc[None],
        total[:H], total[H : 2 * H], total[2 * H : 3 * H],
    )


def build(split):
    held = P(DP, SEQ, None)
    return jax.shard_map(
        on_device,
        mesh=split,
        in_specs=(held, held, held, held, P(), P(), P(), held),
        out_specs=(held, held, held, held, P(), P(), P()),
        check_vma=False,
    )


def solution(mesh):
    return build(Mesh(mesh.devices.reshape(2, 4, 2, 8, 2), SEQ_DP))
```

```python
import functools
import math

import jax
import jax.numpy as jnp
from jax import lax
from jax.experimental import pallas as pl
from jax.experimental.pallas import tpu as pltpu
from jax.sharding import Mesh
from jax.sharding import PartitionSpec as P

SEQ = ("seq_0", "seq_1")
DP = ("dp_0", "dp_1", "dp_2")
SEQ_DP = ("seq_0", "seq_1", "dp_0", "dp_1", "dp_2")

F32 = jnp.float32
BF16 = jnp.bfloat16
LOG2E = math.log2(math.e)
T = 256
H = 40
HP = 2560
N = 128
DEV = 8
ROWS = N // DEV
STEP = 512
STEPS = HP // STEP
TOP = 7.0
TINY = 1e-30


def halves(value):
    high = value.astype(BF16)
    return high, (value - high.astype(F32)).astype(BF16)


def twice(rows):
    return jnp.concatenate([rows, rows], axis=1)


def stacked(value):
    return jnp.concatenate(halves(value), axis=0)


def dot(a, b):
    return jnp.dot(a, b, preferred_element_type=F32)


def dot_nt(a, b):
    return lax.dot_general(a, b, (((1,), (1,)), ((), ())), preferred_element_type=F32)


def in_three(value):
    high = value.astype(BF16).astype(F32)
    mid = (value - high).astype(BF16).astype(F32)
    return jnp.concatenate([high, mid, value - high - mid], axis=0).astype(BF16)


def summed_by(value, zero_one):
    out = dot(in_three(value), zero_one)
    n = value.shape[0]
    return out[:n] + out[n : 2 * n] + out[2 * n :]


def iota(shape, dim):
    return lax.broadcasted_iota(jnp.int32, shape, dim)


def spread(columns, k, count):
    first = iota((T, 128), 1) < 64
    pairs = [
        jnp.where(first, columns[:, j : j + 1], columns[:, j + 1 : j + 2])
        for j in range(k, k + count, 2)
    ]
    return jnp.concatenate(pairs, axis=1)


def exponent(bound):
    return jnp.ceil(jnp.log2(bound + TINY)) - TOP


def prepare(raw_hbm, dlog_hbm, bias_hbm, x_hbm, g_hbm, b_hbm, c_hbm,
            msg_ref, scale_ref, ext_ref, col_hbm, row_hbm, fin_hbm,
            raw_ref, dlog_ref, bias_ref, x_ref, g_ref, b_ref, c_ref, col_ref, row_ref, fin_ref,
            sems, wide, peaks):
    results = [
        pltpu.make_async_copy(source, target, sems.at[7 + k])
        for k, (source, target) in enumerate((
            (col_ref, col_hbm), (row_ref, row_hbm), (fin_ref, fin_hbm),
        ))
    ]
    copies = [
        pltpu.make_async_copy(source, target, sems.at[k])
        for k, (source, target) in enumerate((
            (raw_hbm, raw_ref), (dlog_hbm, dlog_ref), (bias_hbm, bias_ref), (b_hbm, b_ref),
            (x_hbm, x_ref), (c_hbm, c_ref), (g_hbm, g_ref),
        ))
    ]
    for copy in copies:
        copy.start()
    for copy in copies[:3]:
        copy.wait()
    peaks[0:8] = jnp.zeros((8, 128), F32)
    peaks[0:1, :H] = jnp.exp(dlog_ref[...])
    peaks[1:2, :H] = bias_ref[...]
    heads = jnp.concatenate([peaks[0:8], jnp.zeros((120, 128), F32)], axis=0).T[:H]
    v = raw_ref[...].astype(F32) + heads[:, 1:2]
    dt = jnp.maximum(v, 0.0) + jnp.log1p(jnp.exp(-jnp.abs(v)))
    la = -heads[:, 0:1] * dt
    fin_ref[0] = dt
    fin_ref[1] = 1.0 / (1.0 + jnp.exp(-v))
    fin_ref[2] = la
    until = (iota((T, T), 0) <= iota((T, T), 1)).astype(BF16)
    run = summed_by(la, until) * LOG2E
    row_ref[...] = run
    total = run[:, T - 1 : T]
    wide[0:H] = run - jnp.log2(dt)
    wide[H : 2 * H] = fin_ref[3] = jnp.exp2(total - run) * dt
    wide[2 * H : 3 * H] = fin_ref[4] = jnp.exp2(run)
    wide[3 * H :] = jnp.zeros((128 - 3 * H, T), F32)
    columns = wide[...].T
    for i in range(STEPS):
        for part in range(3):
            at = H * part + 8 * i
            col_ref[i, :, 8 * part : 8 * part + 8] = columns[:, at : at + 8]
    for result in results:
        result.start()
    keep = columns[T - 1 : T, 2 * H : 3 * H]
    keep_a = keep.astype(BF16).astype(F32)
    keep_b = (keep - keep_a).astype(BF16).astype(F32)
    keep_c = keep - keep_a - keep_b
    ext_ref[...] = jnp.zeros_like(ext_ref)
    ext_ref[0:1, :H] = keep_a
    ext_ref[1:2, :H] = keep_b * 512.0
    ext_ref[2:3, :H] = keep_c * 262144.0
    peaks[...] = jnp.zeros_like(peaks)
    for r, (source, start, maps) in enumerate(((x_ref, H, b_ref), (g_ref, 2 * H, c_ref))):
        copies[3 + 2 * r].wait()
        copies[4 + 2 * r].wait()
        left = twice(maps[...].astype(F32).T.astype(BF16))
        for j in range(HP // 256):
            lanes = slice(256 * j, 256 * j + 256)
            weight = spread(columns, start + 4 * j, 4)
            state = dot(left, stacked(source[:, lanes].astype(F32) * weight))
            most = jnp.max(jnp.abs(state), axis=0, keepdims=True)
            peaks[24 * r + 2 * j : 24 * r + 2 * j + 1] = most[:, :128]
            peaks[24 * r + 2 * j + 1 : 24 * r + 2 * j + 2] = most[:, 128:]
            for o in range(DEV):
                msg_ref[o, ROWS * r : ROWS * r + ROWS, lanes] = state[ROWS * o : ROWS * o + ROWS]
    lane = iota((24, 128), 1)
    pair = 2 * iota((24, 128), 0)
    for r in range(2):
        most = peaks[24 * r : 24 * r + 24]
        even = exponent(jnp.max(jnp.where(lane < 64, most, 0.0), axis=1, keepdims=True))
        odd = exponent(jnp.max(jnp.where(lane < 64, 0.0, most), axis=1, keepdims=True))
        placed = jnp.where(lane == pair, even, jnp.where(lane == pair + 1, odd, 0.0))
        ext_ref[3 + r : 4 + r] = jnp.sum(placed, axis=0, keepdims=True)
        scale = jnp.exp2(-jnp.where(lane < 64, even, odd))
        for j in range(HP // 128):
            scale_ref[r : r + 1, 128 * j : 128 * j + 128] = scale[j : j + 1]
    for result in results:
        result.wait()


def scan(got_ref, extra_ref, out_ref, ext_ref, wide):
    extra = [extra_ref[j] for j in range(DEV)]
    keep = [e[0:1] + e[1:2] * (1.0 / 512.0) + e[2:3] * (1.0 / 262144.0) for e in extra]
    in_s = [jnp.exp2(e[3:4]) for e in extra]
    in_g = [jnp.exp2(e[4:5]) for e in extra]
    top = 2.0**TOP
    zero = jnp.zeros((1, 128), F32)
    bound_s, bound_g = [zero], [zero]
    for k in range(DEV - 1):
        bound_s.append(keep[k] * bound_s[-1] + in_s[k] * top)
        back = DEV - 1 - k
        bound_g.append(keep[back] * bound_g[-1] + in_g[back] * top)
    bound_g = bound_g[::-1]
    exp_s = [exponent(b) for b in bound_s]
    exp_g = [exponent(b) for b in bound_g]
    for k in range(DEV):
        ext_ref[k, 0:1] = exp_s[k]
        ext_ref[k, 1:2] = exp_g[k]
        ext_ref[k, 2:8] = jnp.zeros((6, 128), F32)
    rows = keep + in_s + in_g + [jnp.exp2(-e) for e in exp_s] + [jnp.exp2(-e) for e in exp_g]
    rows = jnp.concatenate(rows, axis=0)
    parts = in_three(rows)
    count = 5 * DEV
    for c in range(STEPS):
        lanes = slice(STEP * c, STEP * c + STEP)
        hot = (iota((128, STEP), 0) == (iota((128, STEP), 1) + STEP * c) // 64).astype(BF16)
        over = dot(parts, hot)
        wide[:, lanes] = over[:count] + over[count : 2 * count] + over[2 * count :]
    for c in range(STEPS):
        lanes = slice(STEP * c, STEP * c + STEP)
        for first, scale, out, order in (
            (0, DEV, 3 * DEV, range(DEV)),
            (ROWS, 2 * DEV, 4 * DEV, range(DEV - 1, -1, -1)),
        ):
            held = jnp.zeros((ROWS, STEP), F32)
            for k in order:
                here = slice(first, first + ROWS)
                out_ref[k, here, lanes] = held * wide[out + k : out + k + 1, lanes]
                held = (
                    wide[k : k + 1, lanes] * held
                    + wide[scale + k : scale + k + 1, lanes] * got_ref[k, here, lanes]
                )


def inside(x_ref, g_ref, b_ref, c_ref, col_ref, row_ref,
           dx_ref, qrow_ref, qcol_ref, gx_ref, db_ref, dc_ref, score, total, qcol):
    i = pl.program_id(0)
    half = T // 2

    @pl.when(i == 0)
    def _():
        score[...] = dot_nt(b_ref[...], c_ref[...])
        total[...] = jnp.zeros_like(total)
        qcol[...] = jnp.zeros_like(qcol)

    causal = iota((half, T), 1) >= iota((half, T), 0)
    causal_end = iota((half, half), 1) >= iota((half, half), 0)
    lane = iota((half, 128), 1)
    for p in range(STEP // 128):
        lanes = slice(128 * p, 128 * p + 128)
        x = x_ref[:, lanes]
        g = g_ref[:, lanes]
        gx = jnp.sum(x.astype(F32) * g.astype(F32), axis=0, keepdims=True)
        gx_ref[:, lanes] = gx
        grads = []
        for q in range(2):
            k = 2 * p + q
            mine = iota((T, 128), 1) < 64 if q == 0 else iota((T, 128), 1) >= 64
            own = jnp.where(mine, x, jnp.zeros_like(x))
            at = 8 * i + k
            parts = []
            sums = []
            for start, width, keep in ((0, T, causal), (half, half, causal_end)):
                here = slice(start, start + half)
                later = slice(T - width, T)
                gap = row_ref[k : k + 1, later] - col_ref[0, here, k : k + 1]
                decay = jnp.exp2(jnp.where(keep, gap, -1e5))
                cross = dot_nt(own[here], g[later])
                weight = decay * score[here, later]
                high, low = halves(weight)
                parts.append(dot(high, g[later]) + dot(low, g[later]))
                total[here, later] += decay * cross
                pair = weight * cross
                sums.append(jnp.sum(pair, axis=0, keepdims=True))
                qcol[here] += jnp.where(lane == at, jnp.sum(pair, axis=1, keepdims=True), 0.0)
            qrow_ref[k : k + 1, :half] = sums[0][:, :half]
            qrow_ref[k : k + 1, half:] = sums[0][:, half:] + sums[1]
            grads.append(parts)
        for s in range(2):
            dx_ref[half * s : half * s + half, lanes] = jnp.where(
                lane < 64, grads[0][s], grads[1][s]
            )

    @pl.when(i == STEPS - 1)
    def _():
        high, low = halves(total[...])
        db_ref[...] = dot(high, c_ref[...]) + dot(low, c_ref[...])
        high, low = halves(total[...].T)
        dc_ref[...] = dot(high, b_ref[...]) + dot(low, b_ref[...])
        qcol_ref[...] = qcol[...].T[:H]


def entering(got_ref, first, i):
    lanes = slice(STEP * i, STEP * i + STEP)
    return jnp.concatenate([got_ref[o, first : first + ROWS, lanes] for o in range(DEV)], axis=0)


def outside(x_hbm, g_hbm, b_ref, c_ref, got_ref, all_ref, qrow_ref, qcol_ref, gx_ref,
            fin_ref, keep_ref, steps_ref, par_ref, x_ref, g_ref, sems, far_row, far_col):
    copies = [
        pltpu.make_async_copy(g_hbm, g_ref, sems.at[0]),
        pltpu.make_async_copy(x_hbm, x_ref, sems.at[1]),
    ]
    for copy in copies:
        copy.start()
    lane_sums = jnp.zeros((16, 128), F32)
    b_two, c_two = twice(b_ref[...]), twice(c_ref[...])
    lane = iota((T, 128), 1)
    far_col[...] = jnp.zeros_like(far_col)
    for i in range(STEPS):
        whole = slice(STEP * i, STEP * i + STEP)
        state, slope = entering(got_ref, 0, i), entering(got_ref, ROWS, i)
        seen = dot(c_two, stacked(state))
        back = dot(b_two, stacked(slope))
        hot = (iota((STEP, 128), 1) == iota((STEP, 128), 0) // 64 + 8 * i).astype(BF16)
        both = jnp.concatenate(
            [jnp.sum(state * slope, axis=0, keepdims=True), gx_ref[:, whole],
             jnp.zeros((14, STEP), F32)],
            axis=0,
        )
        if i == 0:
            copies[0].wait()
        rows = g_ref[:, whole].astype(F32) * seen
        if i == 0:
            copies[1].wait()
        cols = x_ref[:, whole].astype(F32) * back
        out = dot(jnp.concatenate([stacked(rows), in_three(both)], axis=0), hot)
        rows = out[0:T] + out[T : 2 * T]
        far_row[...] = rows if i == 0 else far_row[...] + rows
        held = far_col[...]
        for p in range(STEP // 128):
            part = cols[:, 128 * p : 128 * p + 128]
            even = jnp.sum(jnp.where(lane < 64, part, 0.0), axis=1, keepdims=True)
            odd = jnp.sum(jnp.where(lane < 64, 0.0, part), axis=1, keepdims=True)
            at = 8 * i + 2 * p
            held = jnp.where(lane == at, even, jnp.where(lane == at + 1, odd, held))
        far_col[...] = held
        last = out[2 * T :]
        lane_sums += last[0:16] + last[16:32] + last[32:48]
    dt, gate, la = fin_ref[0], fin_ref[1], fin_ref[2]
    keep = keep_ref[0:1] + keep_ref[1:2] * (1.0 / 512.0) + keep_ref[2:3] * (1.0 / 262144.0)
    scale_s, scale_g = jnp.exp2(all_ref[0:1]), jnp.exp2(all_ref[1:2])
    ends = keep * scale_s * lane_sums[0:1] * scale_g
    by_head = jnp.concatenate([ends, scale_s, scale_g, jnp.zeros((125, 128), F32)], axis=0).T[:H]
    rows = far_row[...].T[:H] * (fin_ref[4] * by_head[:, 1:2])
    cols = far_col[...].T[:H] * (fin_ref[3] * by_head[:, 2:3])
    since = (iota((T, T), 0) >= iota((T, T), 1)).astype(BF16)
    before = (iota((T, T), 0) < iota((T, T), 1)).astype(BF16)
    summed = summed_by(qrow_ref[...] - qcol_ref[...] + rows, since) + summed_by(cols, before)
    rate = la * (summed + by_head[:, 0:1])
    grad = gate * ((qcol_ref[...] + cols + rate) / dt)
    steps_ref[...] = grad
    sums = dot_nt(jnp.ones((8, T), BF16), in_three(jnp.concatenate([rate, grad], axis=0)))[0:1]
    sums = sums[:, : 2 * H] + sums[:, 2 * H : 4 * H] + sums[:, 4 * H :]
    mine = jnp.concatenate(
        [sums[:, :H], lane_sums[1:2, :H], sums[:, H:], jnp.zeros((1, 128 - 3 * H), F32)], axis=1
    )
    par_ref[...] = jnp.broadcast_to(mine[None], par_ref.shape)


def maps(x_hbm, g_hbm, b_hbm, col_hbm, db_hbm, dc_hbm, near_hbm, got_ref, all_ref, skip_ref,
         dx_hbm, db_ref, dc_ref, x_ref, g_ref, b_ref, col_ref, near_ref, part_ref, dx_ref, sems):
    copies = [
        pltpu.make_async_copy(source, target, sems.at[k])
        for k, (source, target) in enumerate((
            (col_hbm, col_ref), (b_hbm, b_ref), (x_hbm, x_ref), (db_hbm, db_ref),
            (g_hbm, g_ref), (dc_hbm, dc_ref), (near_hbm, near_ref),
        ))
    ]
    leave = pltpu.make_async_copy(dx_ref, dx_hbm, sems.at[len(copies)])
    for copy in copies:
        copy.start()
    for copy in copies[:4]:
        copy.wait()
    b_two = twice(b_ref[...])
    first = iota((1, 128), 1) < 64

    def gained(rows, weight, other):
        out = dot_nt(stacked(weight * rows), stacked(other))
        return out[:T, :N] + out[:T, N:] + out[T:, :N]

    for i in range(STEPS):
        whole = slice(STEP * i, STEP * i + STEP)
        at = slice(8 * i, 8 * i + 8)
        into = spread(col_ref[i, :, 8:16] * jnp.exp2(all_ref[1:2, at]), 0, 8)
        slope = entering(got_ref, ROWS, i)
        part_ref[:, whole] = into * dot(b_two, stacked(slope))
        db_ref[...] += gained(x_ref[:, whole].astype(F32), into, slope)
    for copy in copies[4:]:
        copy.wait()
    for i in range(STEPS):
        whole = slice(STEP * i, STEP * i + STEP)
        g = g_ref[:, whole].astype(F32)
        skip = jnp.concatenate(
            [jnp.where(first, skip_ref[k], skip_ref[k + 1]) for k in range(8 * i, 8 * i + 8, 2)],
            axis=1,
        )
        dx_ref[:, whole] = (near_ref[:, whole] + part_ref[:, whole] + skip * g).astype(BF16)
    leave.start()
    for i in range(STEPS):
        at = slice(8 * i, 8 * i + 8)
        outof = spread(col_ref[i, :, 16:24] * jnp.exp2(all_ref[0:1, at]), 0, 8)
        g = g_ref[:, STEP * i : STEP * i + STEP].astype(F32)
        dc_ref[...] += gained(g, outof, entering(got_ref, 0, i))
    leave.wait()


def spec(shape, index=None):
    index = index or (lambda i: (0,) * len(shape))
    return pl.BlockSpec(shape, index)


def shape(*dims, dtype=F32):
    return jax.ShapeDtypeStruct(dims, dtype)


def coded(body):
    return (body * jnp.abs(body)).astype(jnp.float16)


def decoded(body):
    body = body.astype(F32)
    return near(body * lax.rsqrt(jnp.maximum(jnp.abs(body), TINY)))


def near(array):
    return pltpu.with_memory_space_constraint(array, pltpu.VMEM)


def far_off(*arrays):
    return [pltpu.with_memory_space_constraint(a, pltpu.HBM) for a in arrays]


def exchange(message):
    return lax.all_to_all(message, SEQ, 0, 0, tiled=True)


def on_device(
    tokens_in, step_raw, input_map, output_map, decay_log, skip_gain, step_bias, grad_out
):
    x, raw, b, c, g = (m[0] for m in (tokens_in, step_raw, input_map, output_map, grad_out))
    ranks = lax.axis_size(SEQ) * lax.axis_size(DP)
    factor = 1.0 / math.sqrt(ranks * T * (HP // H))
    vmem = pl.BlockSpec(memory_space=pltpu.VMEM)
    cost = pl.CostEstimate(
        flops=4_000_000_000, bytes_accessed=8_000_000, transcendentals=2_000_000
    )
    room = pltpu.CompilerParams(vmem_limit_bytes=24 * 1024 * 1024)
    msg, scale, ext, cols, rows, fin = pl.pallas_call(
        prepare,
        in_specs=(pl.BlockSpec(memory_space=pltpu.HBM),) * 7,
        out_shape=(
            pltpu.VMEM((DEV, 2 * ROWS, HP), F32), pltpu.VMEM((2, HP), F32),
            pltpu.VMEM((8, 128), F32), pltpu.HBM((STEPS, T, 24), F32), pltpu.HBM((H, T), F32),
            pltpu.HBM((5, H, T), F32),
        ),
        out_specs=(vmem,) * 3 + (pl.BlockSpec(memory_space=pltpu.HBM),) * 3,
        scratch_shapes=[
            pltpu.VMEM((H, T), BF16), pltpu.VMEM((1, H), F32), pltpu.VMEM((1, H), F32),
            pltpu.VMEM((T, HP), BF16), pltpu.VMEM((T, HP), BF16), pltpu.VMEM((T, N), BF16),
            pltpu.VMEM((T, N), BF16), pltpu.VMEM((STEPS, T, 24), F32), pltpu.VMEM((H, T), F32),
            pltpu.VMEM((5, H, T), F32), pltpu.SemaphoreType.DMA((10,)),
            pltpu.VMEM((128, T), F32), pltpu.VMEM((48, 128), F32),
        ],
        compiler_params=room,
        name="prepare",
    )(*far_off(raw.T, decay_log[None], step_bias[None], x, g, b, c))
    scale = jnp.broadcast_to(scale[:, None], (2, ROWS, HP)).reshape(2 * ROWS, HP)
    extra = jnp.pad(ext, ((0, 2 * ROWS - 8), (0, 0))).astype(jnp.float16)
    extra = jnp.broadcast_to(extra[None], (DEV, 2 * ROWS, 128))
    got = exchange(jnp.concatenate([coded(msg * scale[None]), extra], axis=2))
    got, got_ext = decoded(got[:, :, :HP]), got[:, 0:8, HP:].astype(F32)

    lanes = spec((T, STEP), lambda i: (0, i))
    full = spec((T, N))
    heads = spec((H, T))
    cols_spec = spec((1, T, 24), lambda i: (i, 0, 0))
    gx_spec = spec((1, STEP), lambda i: (0, i))
    near_dx, qrow, qcol, gx, db, dc = pl.pallas_call(
        inside,
        grid=(STEPS,),
        in_specs=[lanes, lanes, full, full, cols_spec, spec((8, T), lambda i: (i, 0))],
        out_specs=[lanes, spec((8, T), lambda i: (i, 0)), heads, gx_spec, full, full],
        out_shape=(
            pltpu.HBM((T, HP), F32), pltpu.HBM((H, T), F32), pltpu.HBM((H, T), F32),
            pltpu.HBM((1, HP), F32), pltpu.HBM((T, N), F32), pltpu.HBM((T, N), F32),
        ),
        scratch_shapes=[
            pltpu.VMEM((T, T), F32), pltpu.VMEM((T, T), F32), pltpu.VMEM((T, 128), F32),
        ],
        cost_estimate=cost,
        compiler_params=room,
        name="inside",
    )(x, g, b, c, cols, rows)

    sent, sent_ext = pl.pallas_call(
        scan,
        in_specs=(vmem, vmem),
        out_shape=(pltpu.VMEM((DEV, 2 * ROWS, HP), F32), pltpu.VMEM((DEV, 8, 128), F32)),
        out_specs=(vmem, vmem),
        scratch_shapes=[pltpu.VMEM((5 * DEV, HP), F32)],
        compiler_params=room,
        name="scan",
    )(got, got_ext)
    back = decoded(exchange(coded(sent)))
    scales = lax.dynamic_index_in_dim(sent_ext, lax.axis_index(SEQ), 0, keepdims=False)

    hbm = pl.BlockSpec(memory_space=pltpu.HBM)
    smem = pl.BlockSpec(memory_space=pltpu.SMEM)
    steps, everyone = pl.pallas_call(
        outside,
        in_specs=[hbm] * 2 + [vmem] * 9,
        out_specs=[vmem] * 2,
        out_shape=(shape(H, T), shape(ranks, 1, 128)),
        scratch_shapes=[
            pltpu.VMEM((T, HP), BF16), pltpu.VMEM((T, HP), BF16), pltpu.SemaphoreType.DMA((2,)),
            pltpu.VMEM((T, 128), F32), pltpu.VMEM((T, 128), F32),
        ],
        compiler_params=room,
        name="outside",
    )(*far_off(x, g), near(b), near(c), back, near(scales), near(qrow), near(qcol),
      near(gx), near(fin), near(ext))
    everyone = lax.all_to_all(everyone, SEQ_DP, 0, 0, tiled=True)
    dx, db, dc = pl.pallas_call(
        maps,
        in_specs=[hbm] * 7 + [vmem] * 2 + [smem],
        out_specs=[hbm, vmem, vmem],
        out_shape=(pltpu.HBM((T, HP), BF16), shape(T, N), shape(T, N)),
        scratch_shapes=[
            pltpu.VMEM((T, HP), BF16), pltpu.VMEM((T, HP), BF16), pltpu.VMEM((T, N), BF16),
            pltpu.VMEM((STEPS, T, 24), F32), pltpu.VMEM((T, HP), F32), pltpu.VMEM((T, HP), F32),
            pltpu.VMEM((T, HP), BF16), pltpu.SemaphoreType.DMA((8,)),
        ],
        cost_estimate=cost,
        compiler_params=room,
        name="maps",
    )(*far_off(x, g, b, cols, db, dc, near_dx), back, near(scales), skip_gain)
    total = jnp.sum(everyone, axis=(0, 1)) * factor
    return (
        dx[None], steps.T[None], db[None], dc[None],
        total[:H], total[H : 2 * H], total[2 * H : 3 * H],
    )


def build(split):
    held = P(DP, SEQ, None)
    return jax.shard_map(
        on_device,
        mesh=split,
        in_specs=(held, held, held, held, P(), P(), P(), held),
        out_specs=(held, held, held, held, P(), P(), P()),
        check_vma=False,
    )


def solution(mesh):
    return build(Mesh(mesh.devices.reshape(2, 4, 2, 8, 2), SEQ_DP))
```

```python
import functools
import math

import jax
import jax.numpy as jnp
from jax import lax
from jax.experimental import pallas as pl
from jax.experimental.pallas import tpu as pltpu
from jax.sharding import Mesh
from jax.sharding import PartitionSpec as P

SEQ = ("seq_0", "seq_1")
DP = ("dp_0", "dp_1", "dp_2")
SEQ_DP = ("seq_0", "seq_1", "dp_0", "dp_1", "dp_2")

F32 = jnp.float32
BF16 = jnp.bfloat16
LOG2E = math.log2(math.e)
T = 256
H = 40
HP = 2560
N = 128
DEV = 8
ROWS = N // DEV
STEP = 512
STEPS = HP // STEP
TOP = 7.0
TINY = 1e-30


def halves(value):
    high = value.astype(BF16)
    return high, (value - high.astype(F32)).astype(BF16)


def twice(rows):
    return jnp.concatenate([rows, rows], axis=1)


def stacked(value):
    return jnp.concatenate(halves(value), axis=0)


def dot(a, b):
    return jnp.dot(a, b, preferred_element_type=F32)


def dot_nt(a, b):
    return lax.dot_general(a, b, (((1,), (1,)), ((), ())), preferred_element_type=F32)


def in_three(value):
    high = value.astype(BF16).astype(F32)
    mid = (value - high).astype(BF16).astype(F32)
    return jnp.concatenate([high, mid, value - high - mid], axis=0).astype(BF16)


def summed_by(value, zero_one):
    out = dot(in_three(value), zero_one)
    n = value.shape[0]
    return out[:n] + out[n : 2 * n] + out[2 * n :]


def iota(shape, dim):
    return lax.broadcasted_iota(jnp.int32, shape, dim)


def spread(columns, k, count):
    first = iota((T, 128), 1) < 64
    pairs = [
        jnp.where(first, columns[:, j : j + 1], columns[:, j + 1 : j + 2])
        for j in range(k, k + count, 2)
    ]
    return jnp.concatenate(pairs, axis=1)


def exponent(bound):
    return jnp.ceil(jnp.log2(bound + TINY)) - TOP


def prepare(raw_hbm, dlog_hbm, bias_hbm, x_hbm, g_hbm, b_hbm, c_hbm,
            msg_ref, scale_ref, ext_ref, col_hbm, row_hbm, fin_hbm,
            raw_ref, dlog_ref, bias_ref, x_ref, g_ref, b_ref, c_ref, col_ref, row_ref, fin_ref,
            sems, wide, peaks):
    results = [
        pltpu.make_async_copy(source, target, sems.at[7 + k])
        for k, (source, target) in enumerate((
            (col_ref, col_hbm), (row_ref, row_hbm), (fin_ref, fin_hbm),
        ))
    ]
    copies = [
        pltpu.make_async_copy(source, target, sems.at[k])
        for k, (source, target) in enumerate((
            (raw_hbm, raw_ref), (dlog_hbm, dlog_ref), (bias_hbm, bias_ref), (b_hbm, b_ref),
            (x_hbm, x_ref), (c_hbm, c_ref), (g_hbm, g_ref),
        ))
    ]
    for copy in copies:
        copy.start()
    for copy in copies[:3]:
        copy.wait()
    peaks[0:8] = jnp.zeros((8, 128), F32)
    peaks[0:1, :H] = jnp.exp(dlog_ref[...])
    peaks[1:2, :H] = bias_ref[...]
    heads = jnp.concatenate([peaks[0:8], jnp.zeros((120, 128), F32)], axis=0).T[:H]
    v = raw_ref[...].astype(F32) + heads[:, 1:2]
    dt = jnp.maximum(v, 0.0) + jnp.log1p(jnp.exp(-jnp.abs(v)))
    la = -heads[:, 0:1] * dt
    fin_ref[0] = dt
    fin_ref[1] = 1.0 / (1.0 + jnp.exp(-v))
    fin_ref[2] = la
    until = (iota((T, T), 0) <= iota((T, T), 1)).astype(BF16)
    run = summed_by(la, until) * LOG2E
    row_ref[...] = run
    total = run[:, T - 1 : T]
    wide[0:H] = run - jnp.log2(dt)
    wide[H : 2 * H] = fin_ref[3] = jnp.exp2(total - run) * dt
    wide[2 * H : 3 * H] = fin_ref[4] = jnp.exp2(run)
    wide[3 * H :] = jnp.zeros((128 - 3 * H, T), F32)
    columns = wide[...].T
    for i in range(STEPS):
        for part in range(3):
            at = H * part + 8 * i
            col_ref[i, :, 8 * part : 8 * part + 8] = columns[:, at : at + 8]
    for result in results:
        result.start()
    keep = columns[T - 1 : T, 2 * H : 3 * H]
    keep_a = keep.astype(BF16).astype(F32)
    keep_b = (keep - keep_a).astype(BF16).astype(F32)
    keep_c = keep - keep_a - keep_b
    ext_ref[...] = jnp.zeros_like(ext_ref)
    ext_ref[0:1, :H] = keep_a
    ext_ref[1:2, :H] = keep_b * 512.0
    ext_ref[2:3, :H] = keep_c * 262144.0
    peaks[...] = jnp.zeros_like(peaks)
    for r, (source, start, maps) in enumerate(((x_ref, H, b_ref), (g_ref, 2 * H, c_ref))):
        copies[3 + 2 * r].wait()
        copies[4 + 2 * r].wait()
        left = twice(maps[...].astype(F32).T.astype(BF16))
        for j in range(HP // 256):
            lanes = slice(256 * j, 256 * j + 256)
            weight = spread(columns, start + 4 * j, 4)
            state = dot(left, stacked(source[:, lanes].astype(F32) * weight))
            most = jnp.max(jnp.abs(state), axis=0, keepdims=True)
            peaks[24 * r + 2 * j : 24 * r + 2 * j + 1] = most[:, :128]
            peaks[24 * r + 2 * j + 1 : 24 * r + 2 * j + 2] = most[:, 128:]
            for o in range(DEV):
                msg_ref[o, ROWS * r : ROWS * r + ROWS, lanes] = state[ROWS * o : ROWS * o + ROWS]
    lane = iota((24, 128), 1)
    pair = 2 * iota((24, 128), 0)
    for r in range(2):
        most = peaks[24 * r : 24 * r + 24]
        even = exponent(jnp.max(jnp.where(lane < 64, most, 0.0), axis=1, keepdims=True))
        odd = exponent(jnp.max(jnp.where(lane < 64, 0.0, most), axis=1, keepdims=True))
        placed = jnp.where(lane == pair, even, jnp.where(lane == pair + 1, odd, 0.0))
        ext_ref[3 + r : 4 + r] = jnp.sum(placed, axis=0, keepdims=True)
        scale = jnp.exp2(-jnp.where(lane < 64, even, odd))
        for j in range(HP // 128):
            scale_ref[r : r + 1, 128 * j : 128 * j + 128] = scale[j : j + 1]
    scale_ref[:, HP:] = jnp.ones((2, 128), F32)
    for o in range(DEV):
        msg_ref[o, 0:8, HP:] = ext_ref[...]
        msg_ref[o, 8:, HP:] = jnp.zeros((2 * ROWS - 8, 128), F32)
    for result in results:
        result.wait()


def scan(got_ref, extra_ref, out_ref, ext_ref, wide):
    extra = [extra_ref[j] for j in range(DEV)]
    keep = [e[0:1] + e[1:2] * (1.0 / 512.0) + e[2:3] * (1.0 / 262144.0) for e in extra]
    in_s = [jnp.exp2(e[3:4]) for e in extra]
    in_g = [jnp.exp2(e[4:5]) for e in extra]
    top = 2.0**TOP
    zero = jnp.zeros((1, 128), F32)
    bound_s, bound_g = [zero], [zero]
    for k in range(DEV - 1):
        bound_s.append(keep[k] * bound_s[-1] + in_s[k] * top)
        back = DEV - 1 - k
        bound_g.append(keep[back] * bound_g[-1] + in_g[back] * top)
    bound_g = bound_g[::-1]
    exp_s = [exponent(b) for b in bound_s]
    exp_g = [exponent(b) for b in bound_g]
    for k in range(DEV):
        ext_ref[k, 0:1] = exp_s[k]
        ext_ref[k, 1:2] = exp_g[k]
        ext_ref[k, 2:8] = jnp.zeros((6, 128), F32)
    rows = keep + in_s + in_g + [jnp.exp2(-e) for e in exp_s] + [jnp.exp2(-e) for e in exp_g]
    rows = jnp.concatenate(rows, axis=0)
    parts = in_three(rows)
    count = 5 * DEV
    for c in range(STEPS):
        lanes = slice(STEP * c, STEP * c + STEP)
        hot = (iota((128, STEP), 0) == (iota((128, STEP), 1) + STEP * c) // 64).astype(BF16)
        over = dot(parts, hot)
        wide[:, lanes] = over[:count] + over[count : 2 * count] + over[2 * count :]
    for c in range(STEPS):
        lanes = slice(STEP * c, STEP * c + STEP)
        for first, scale, out, order in (
            (0, DEV, 3 * DEV, range(DEV)),
            (ROWS, 2 * DEV, 4 * DEV, range(DEV - 1, -1, -1)),
        ):
            held = jnp.zeros((ROWS, STEP), F32)
            for k in order:
                here = slice(first, first + ROWS)
                out_ref[k, here, lanes] = held * wide[out + k : out + k + 1, lanes]
                held = (
                    wide[k : k + 1, lanes] * held
                    + wide[scale + k : scale + k + 1, lanes] * got_ref[k, here, lanes]
                )


def inside(x_ref, g_ref, b_ref, c_ref, col_ref, row_ref,
           dx_ref, qrow_ref, qcol_ref, gx_ref, db_ref, dc_ref, score, total, qcol):
    i = pl.program_id(0)
    half = T // 2

    @pl.when(i == 0)
    def _():
        score[...] = dot_nt(b_ref[...], c_ref[...])
        total[...] = jnp.zeros_like(total)
        qcol[...] = jnp.zeros_like(qcol)

    causal = iota((half, T), 1) >= iota((half, T), 0)
    causal_end = iota((half, half), 1) >= iota((half, half), 0)
    lane = iota((half, 128), 1)
    for p in range(STEP // 128):
        lanes = slice(128 * p, 128 * p + 128)
        x = x_ref[:, lanes]
        g = g_ref[:, lanes]
        gx = jnp.sum(x.astype(F32) * g.astype(F32), axis=0, keepdims=True)
        gx_ref[:, lanes] = gx
        grads = []
        for q in range(2):
            k = 2 * p + q
            mine = iota((T, 128), 1) < 64 if q == 0 else iota((T, 128), 1) >= 64
            own = jnp.where(mine, x, jnp.zeros_like(x))
            at = 8 * i + k
            parts = []
            sums = []
            for start, width, keep in ((0, T, causal), (half, half, causal_end)):
                here = slice(start, start + half)
                later = slice(T - width, T)
                gap = row_ref[k : k + 1, later] - col_ref[0, here, k : k + 1]
                decay = jnp.exp2(jnp.where(keep, gap, -1e5))
                cross = dot_nt(own[here], g[later])
                weight = decay * score[here, later]
                high, low = halves(weight)
                parts.append(dot(high, g[later]) + dot(low, g[later]))
                total[here, later] += decay * cross
                pair = weight * cross
                sums.append(jnp.sum(pair, axis=0, keepdims=True))
                qcol[here] += jnp.where(lane == at, jnp.sum(pair, axis=1, keepdims=True), 0.0)
            qrow_ref[k : k + 1, :half] = sums[0][:, :half]
            qrow_ref[k : k + 1, half:] = sums[0][:, half:] + sums[1]
            grads.append(parts)
        for s in range(2):
            dx_ref[half * s : half * s + half, lanes] = jnp.where(
                lane < 64, grads[0][s], grads[1][s]
            )

    @pl.when(i == STEPS - 1)
    def _():
        high, low = halves(total[...])
        db_ref[...] = dot(high, c_ref[...]) + dot(low, c_ref[...])
        high, low = halves(total[...].T)
        dc_ref[...] = dot(high, b_ref[...]) + dot(low, b_ref[...])
        qcol_ref[...] = qcol[...].T[:H]


def entering(got_ref, first, i):
    lanes = slice(STEP * i, STEP * i + STEP)
    return jnp.concatenate([got_ref[o, first : first + ROWS, lanes] for o in range(DEV)], axis=0)


def outside(x_hbm, g_hbm, b_ref, c_ref, got_ref, all_ref, qrow_ref, qcol_ref, gx_ref,
            fin_ref, keep_ref, steps_ref, par_ref, x_ref, g_ref, sems, far_row, far_col):
    copies = [
        pltpu.make_async_copy(g_hbm, g_ref, sems.at[0]),
        pltpu.make_async_copy(x_hbm, x_ref, sems.at[1]),
    ]
    for copy in copies:
        copy.start()
    lane_sums = jnp.zeros((16, 128), F32)
    b_two, c_two = twice(b_ref[...]), twice(c_ref[...])
    lane = iota((T, 128), 1)
    far_col[...] = jnp.zeros_like(far_col)
    for i in range(STEPS):
        whole = slice(STEP * i, STEP * i + STEP)
        state, slope = entering(got_ref, 0, i), entering(got_ref, ROWS, i)
        seen = dot(c_two, stacked(state))
        back = dot(b_two, stacked(slope))
        hot = (iota((STEP, 128), 1) == iota((STEP, 128), 0) // 64 + 8 * i).astype(BF16)
        both = jnp.concatenate(
            [jnp.sum(state * slope, axis=0, keepdims=True), gx_ref[:, whole],
             jnp.zeros((14, STEP), F32)],
            axis=0,
        )
        if i == 0:
            copies[0].wait()
        rows = g_ref[:, whole].astype(F32) * seen
        if i == 0:
            copies[1].wait()
        cols = x_ref[:, whole].astype(F32) * back
        out = dot(jnp.concatenate([stacked(rows), in_three(both)], axis=0), hot)
        rows = out[0:T] + out[T : 2 * T]
        far_row[...] = rows if i == 0 else far_row[...] + rows
        held = far_col[...]
        for p in range(STEP // 128):
            part = cols[:, 128 * p : 128 * p + 128]
            even = jnp.sum(jnp.where(lane < 64, part, 0.0), axis=1, keepdims=True)
            odd = jnp.sum(jnp.where(lane < 64, 0.0, part), axis=1, keepdims=True)
            at = 8 * i + 2 * p
            held = jnp.where(lane == at, even, jnp.where(lane == at + 1, odd, held))
        far_col[...] = held
        last = out[2 * T :]
        lane_sums += last[0:16] + last[16:32] + last[32:48]
    dt, gate, la = fin_ref[0], fin_ref[1], fin_ref[2]
    keep = keep_ref[0:1] + keep_ref[1:2] * (1.0 / 512.0) + keep_ref[2:3] * (1.0 / 262144.0)
    scale_s, scale_g = jnp.exp2(all_ref[0:1]), jnp.exp2(all_ref[1:2])
    ends = keep * scale_s * lane_sums[0:1] * scale_g
    by_head = jnp.concatenate([ends, scale_s, scale_g, jnp.zeros((125, 128), F32)], axis=0).T[:H]
    rows = far_row[...].T[:H] * (fin_ref[4] * by_head[:, 1:2])
    cols = far_col[...].T[:H] * (fin_ref[3] * by_head[:, 2:3])
    since = (iota((T, T), 0) >= iota((T, T), 1)).astype(BF16)
    before = (iota((T, T), 0) < iota((T, T), 1)).astype(BF16)
    summed = summed_by(qrow_ref[...] - qcol_ref[...] + rows, since) + summed_by(cols, before)
    rate = la * (summed + by_head[:, 0:1])
    grad = gate * ((qcol_ref[...] + cols + rate) / dt)
    steps_ref[...] = grad
    sums = dot_nt(jnp.ones((8, T), BF16), in_three(jnp.concatenate([rate, grad], axis=0)))[0:1]
    sums = sums[:, : 2 * H] + sums[:, 2 * H : 4 * H] + sums[:, 4 * H :]
    mine = jnp.concatenate(
        [sums[:, :H], lane_sums[1:2, :H], sums[:, H:], jnp.zeros((1, 128 - 3 * H), F32)], axis=1
    )
    par_ref[...] = jnp.broadcast_to(mine[None], par_ref.shape)


def maps(x_hbm, g_hbm, b_hbm, col_hbm, db_hbm, dc_hbm, near_hbm, got_ref, all_ref, skip_ref,
         dx_hbm, db_ref, dc_ref, x_ref, g_ref, b_ref, col_ref, near_ref, part_ref, dx_ref, sems):
    copies = [
        pltpu.make_async_copy(source, target, sems.at[k])
        for k, (source, target) in enumerate((
            (col_hbm, col_ref), (b_hbm, b_ref), (x_hbm, x_ref), (db_hbm, db_ref),
            (g_hbm, g_ref), (dc_hbm, dc_ref), (near_hbm, near_ref),
        ))
    ]
    leave = pltpu.make_async_copy(dx_ref, dx_hbm, sems.at[len(copies)])
    for copy in copies:
        copy.start()
    for copy in copies[:4]:
        copy.wait()
    b_two = twice(b_ref[...])
    first = iota((1, 128), 1) < 64

    def gained(rows, weight, other):
        out = dot_nt(stacked(weight * rows), stacked(other))
        return out[:T, :N] + out[:T, N:] + out[T:, :N]

    for i in range(STEPS):
        whole = slice(STEP * i, STEP * i + STEP)
        at = slice(8 * i, 8 * i + 8)
        into = spread(col_ref[i, :, 8:16] * jnp.exp2(all_ref[1:2, at]), 0, 8)
        slope = entering(got_ref, ROWS, i)
        part_ref[:, whole] = into * dot(b_two, stacked(slope))
        db_ref[...] += gained(x_ref[:, whole].astype(F32), into, slope)
    for copy in copies[4:]:
        copy.wait()
    for i in range(STEPS):
        whole = slice(STEP * i, STEP * i + STEP)
        g = g_ref[:, whole].astype(F32)
        skip = jnp.concatenate(
            [jnp.where(first, skip_ref[k], skip_ref[k + 1]) for k in range(8 * i, 8 * i + 8, 2)],
            axis=1,
        )
        dx_ref[:, whole] = (near_ref[:, whole] + part_ref[:, whole] + skip * g).astype(BF16)
    leave.start()
    for i in range(STEPS):
        at = slice(8 * i, 8 * i + 8)
        outof = spread(col_ref[i, :, 16:24] * jnp.exp2(all_ref[0:1, at]), 0, 8)
        g = g_ref[:, STEP * i : STEP * i + STEP].astype(F32)
        dc_ref[...] += gained(g, outof, entering(got_ref, 0, i))
    leave.wait()


def spec(shape, index=None):
    index = index or (lambda i: (0,) * len(shape))
    return pl.BlockSpec(shape, index)


def shape(*dims, dtype=F32):
    return jax.ShapeDtypeStruct(dims, dtype)


def coded(body):
    return (body * jnp.abs(body)).astype(jnp.float16)


def decoded(body):
    body = body.astype(F32)
    return near(body * lax.rsqrt(jnp.maximum(jnp.abs(body), TINY)))


def near(array):
    return pltpu.with_memory_space_constraint(array, pltpu.VMEM)


def far_off(*arrays):
    return [pltpu.with_memory_space_constraint(a, pltpu.HBM) for a in arrays]


def exchange(message):
    return lax.all_to_all(message, SEQ, 0, 0, tiled=True)


def on_device(
    tokens_in, step_raw, input_map, output_map, decay_log, skip_gain, step_bias, grad_out
):
    x, raw, b, c, g = (m[0] for m in (tokens_in, step_raw, input_map, output_map, grad_out))
    ranks = lax.axis_size(SEQ) * lax.axis_size(DP)
    factor = 1.0 / math.sqrt(ranks * T * (HP // H))
    vmem = pl.BlockSpec(memory_space=pltpu.VMEM)
    cost = pl.CostEstimate(
        flops=4_000_000_000, bytes_accessed=8_000_000, transcendentals=2_000_000
    )
    room = pltpu.CompilerParams(vmem_limit_bytes=24 * 1024 * 1024)
    msg, scale, ext, cols, rows, fin = pl.pallas_call(
        prepare,
        in_specs=(pl.BlockSpec(memory_space=pltpu.HBM),) * 7,
        out_shape=(
            pltpu.VMEM((DEV, 2 * ROWS, HP + 128), F32), pltpu.VMEM((2, HP + 128), F32),
            pltpu.VMEM((8, 128), F32), pltpu.HBM((STEPS, T, 24), F32), pltpu.HBM((H, T), F32),
            pltpu.HBM((5, H, T), F32),
        ),
        out_specs=(vmem,) * 3 + (pl.BlockSpec(memory_space=pltpu.HBM),) * 3,
        scratch_shapes=[
            pltpu.VMEM((H, T), BF16), pltpu.VMEM((1, H), F32), pltpu.VMEM((1, H), F32),
            pltpu.VMEM((T, HP), BF16), pltpu.VMEM((T, HP), BF16), pltpu.VMEM((T, N), BF16),
            pltpu.VMEM((T, N), BF16), pltpu.VMEM((STEPS, T, 24), F32), pltpu.VMEM((H, T), F32),
            pltpu.VMEM((5, H, T), F32), pltpu.SemaphoreType.DMA((10,)),
            pltpu.VMEM((128, T), F32), pltpu.VMEM((48, 128), F32),
        ],
        compiler_params=room,
        name="prepare",
    )(*far_off(raw.T, decay_log[None], step_bias[None], x, g, b, c))
    scale = jnp.broadcast_to(scale[:, None], (2, ROWS, HP + 128)).reshape(2 * ROWS, HP + 128)
    msg = msg * scale[None]
    msg = jnp.where(iota(msg.shape, 2) < HP, msg * jnp.abs(msg), msg)
    got = exchange(msg.astype(jnp.float16))
    got, got_ext = decoded(got[:, :, :HP]), got[:, 0:8, HP:].astype(F32)

    lanes = spec((T, STEP), lambda i: (0, i))
    full = spec((T, N))
    heads = spec((H, T))
    cols_spec = spec((1, T, 24), lambda i: (i, 0, 0))
    gx_spec = spec((1, STEP), lambda i: (0, i))
    near_dx, qrow, qcol, gx, db, dc = pl.pallas_call(
        inside,
        grid=(STEPS,),
        in_specs=[lanes, lanes, full, full, cols_spec, spec((8, T), lambda i: (i, 0))],
        out_specs=[lanes, spec((8, T), lambda i: (i, 0)), heads, gx_spec, full, full],
        out_shape=(
            pltpu.HBM((T, HP), F32), pltpu.HBM((H, T), F32), pltpu.HBM((H, T), F32),
            pltpu.HBM((1, HP), F32), pltpu.HBM((T, N), F32), pltpu.HBM((T, N), F32),
        ),
        scratch_shapes=[
            pltpu.VMEM((T, T), F32), pltpu.VMEM((T, T), F32), pltpu.VMEM((T, 128), F32),
        ],
        cost_estimate=cost,
        compiler_params=room,
        name="inside",
    )(x, g, b, c, cols, rows)

    sent, sent_ext = pl.pallas_call(
        scan,
        in_specs=(vmem, vmem),
        out_shape=(pltpu.VMEM((DEV, 2 * ROWS, HP), F32), pltpu.VMEM((DEV, 8, 128), F32)),
        out_specs=(vmem, vmem),
        scratch_shapes=[pltpu.VMEM((5 * DEV, HP), F32)],
        compiler_params=room,
        name="scan",
    )(got, got_ext)
    back = decoded(exchange(coded(sent)))
    scales = lax.dynamic_index_in_dim(sent_ext, lax.axis_index(SEQ), 0, keepdims=False)

    hbm = pl.BlockSpec(memory_space=pltpu.HBM)
    smem = pl.BlockSpec(memory_space=pltpu.SMEM)
    steps, everyone = pl.pallas_call(
        outside,
        in_specs=[hbm] * 2 + [vmem] * 9,
        out_specs=[vmem] * 2,
        out_shape=(shape(H, T), shape(ranks, 1, 128)),
        scratch_shapes=[
            pltpu.VMEM((T, HP), BF16), pltpu.VMEM((T, HP), BF16), pltpu.SemaphoreType.DMA((2,)),
            pltpu.VMEM((T, 128), F32), pltpu.VMEM((T, 128), F32),
        ],
        compiler_params=room,
        name="outside",
    )(*far_off(x, g), near(b), near(c), back, near(scales), near(qrow), near(qcol),
      near(gx), near(fin), near(ext))
    everyone = lax.all_to_all(everyone, SEQ_DP, 0, 0, tiled=True)
    dx, db, dc = pl.pallas_call(
        maps,
        in_specs=[hbm] * 7 + [vmem] * 2 + [smem],
        out_specs=[hbm, vmem, vmem],
        out_shape=(pltpu.HBM((T, HP), BF16), shape(T, N), shape(T, N)),
        scratch_shapes=[
            pltpu.VMEM((T, HP), BF16), pltpu.VMEM((T, HP), BF16), pltpu.VMEM((T, N), BF16),
            pltpu.VMEM((STEPS, T, 24), F32), pltpu.VMEM((T, HP), F32), pltpu.VMEM((T, HP), F32),
            pltpu.VMEM((T, HP), BF16), pltpu.SemaphoreType.DMA((8,)),
        ],
        cost_estimate=cost,
        compiler_params=room,
        name="maps",
    )(*far_off(x, g, b, cols, db, dc, near_dx), back, near(scales), skip_gain)
    total = jnp.sum(everyone, axis=(0, 1)) * factor
    return (
        dx[None], steps.T[None], db[None], dc[None],
        total[:H], total[H : 2 * H], total[2 * H : 3 * H],
    )


def build(split):
    held = P(DP, SEQ, None)
    return jax.shard_map(
        on_device,
        mesh=split,
        in_specs=(held, held, held, held, P(), P(), P(), held),
        out_specs=(held, held, held, held, P(), P(), P()),
        check_vma=False,
    )


def solution(mesh):
    return build(Mesh(mesh.devices.reshape(2, 4, 2, 8, 2), SEQ_DP))
```
